128 devices in a mesh: section: 32 (over y, z, core), tensor: 4 (over x).
Axes of the slice: x: 4, y: 4, z: 4, core: 2. Of those that a mesh axis runs over, the one named last changes fastest.
Arguments:
- section_input: bfloat16 [32, 512, 4096], P('section', 'tensor'), may hold values from -6 to 6
- history: bfloat16 [32, 7, 512, 4096], P('section', None, 'tensor'), may hold values from -6 to 6
- query_weight: bfloat16 [32, 4096, 3072], P('section', None, 'tensor'), may hold values from -0.4 to 0.4
- key_weight: bfloat16 [32, 4096, 512], P('section', None, 'tensor'), may hold values from -0.4 to 0.4
- value_weight: bfloat16 [32, 4096, 512], P('section', None, 'tensor'), may hold values from -0.09375 to 0.09375
- output_weight: bfloat16 [32, 3072, 4096], P('section', 'tensor'), may hold values from -0.5 to 0.5
- mix_weights: float32 [32, 8], replicated, may hold values from 0.2 to 0.6
Outputs:
- next_input: bfloat16 [32, 512, 4096], P('section', 'tensor')
The draws below stay inside these ranges and needn't reach their ends.
All inputs are finite; a program needn't handle non-finite values.
Results may differ from the reference program's by a relative error of at most 0.013.
The reference program's roundings to bfloat16 on the way count: a program that leaves them out, or rounds other values in their place, can miss the bound.
Values may be sent and summed in bfloat16 or wider, within the bound.
A program may use at most 128 MiB of HBM per device.

```python
import math
import jax
import jax.numpy as jnp
from jax import lax

D = 4096
HEADS = 48
KV_HEADS = 8
HEAD_DIM = 64
DILATION_STRIDE = 4
SEQ = 512
HIST = 7
N_SECTION = 32
N_TENSOR = 4


def draw_query_weight(key, part):
    entries = jax.random.normal(jax.random.fold_in(key, 11), (N_SECTION, D, HEADS * HEAD_DIM), jnp.float32) / jnp.sqrt(jnp.float32(D))
    return jnp.clip(entries, -0.39, 0.39).astype(jnp.bfloat16)


def draw_key_weight(key, part):
    entries = jax.random.normal(jax.random.fold_in(key, 13), (N_SECTION, D, KV_HEADS * HEAD_DIM), jnp.float32) / jnp.sqrt(jnp.float32(D))
    return jnp.clip(entries, -0.39, 0.39).astype(jnp.bfloat16)


def steps_of(rng, extent, shards, low, high):
    level, own = 1.0, jax.random.fold_in(rng, 6)
    for dim, shards_of in shards:
        heights = jnp.exp(jax.random.uniform(jax.random.fold_in(own, dim), (shards_of,), jnp.float32, low / len(shards), high / len(shards)))
        level = level * jnp.repeat(heights, extent[dim] // shards_of).reshape([-1 if axis == dim else 1 for axis in range(len(extent))])
    return level


def noise(key, shape, spread, reach, shards=(), kind=jnp.bfloat16):
    factor_of = steps_of(key, shape, shards, -0.22, 0.18) if shards else 1.0
    result = jax.random.normal(key, shape, jnp.float32) * spread * factor_of
    return jnp.minimum(jnp.maximum(result, -reach), reach).astype(kind)


def setup_inputs(seed: int = 0) -> dict:
    seeds = jax.random.split(jax.random.key(seed), 8)
    return {
        "section_input": noise(seeds[0], (N_SECTION, SEQ, D), 1.0, 6.0, ((0, 32), (1, 4))),
        "history": noise(seeds[1], (N_SECTION, HIST, SEQ, D), 1.0, 6.0, ((0, 32), (2, 4))),
        "query_weight": draw_query_weight(jax.random.fold_in(seeds[7], 71), 0),
        "key_weight": draw_key_weight(jax.random.fold_in(seeds[7], 71), 0),
        "value_weight": noise(seeds[4], (N_SECTION, D, KV_HEADS * HEAD_DIM), D ** -0.5, 0.09375, ((0, 32), (2, 4))),
        "output_weight": noise(seeds[5], (N_SECTION, HEADS * HEAD_DIM, D), 0.08, 0.5, ((0, 32), (1, 4))),
        "mix_weights": jnp.clip(jax.random.uniform(seeds[6], (N_SECTION, HIST + 1), jnp.float32, 0.2, 0.6), 0.2, 0.6),
    }


def normalize(token_rows):
    values = token_rows.astype(jnp.float32)
    inv_scale = lax.rsqrt(lax.optimization_barrier(jnp.mean(values * values, axis=-1, keepdims=True)) + 1e-05)
    return (values * inv_scale).astype(jnp.bfloat16)

def one_section(operands):
    token_rows, query_part, key_part, value_part, output_part = operands
    seq_len = token_rows.shape[0]
    normed = normalize(token_rows)
    query_rows = jnp.dot(normed, query_part, preferred_element_type=jnp.float32).astype(jnp.bfloat16)
    key_rows = jnp.dot(normed, key_part, preferred_element_type=jnp.float32).astype(jnp.bfloat16)
    value_rows = jnp.dot(normed, value_part, preferred_element_type=jnp.float32).astype(jnp.bfloat16)
    per_group = HEADS // KV_HEADS
    query_heads = query_rows.astype(jnp.float32).reshape(seq_len, KV_HEADS, per_group, HEAD_DIM)
    key_heads = key_rows.astype(jnp.float32).reshape(seq_len, KV_HEADS, HEAD_DIM)
    value_heads = value_rows.astype(jnp.float32).reshape(seq_len, KV_HEADS, HEAD_DIM)
    scores = jnp.einsum('tgjd,sgd->gjts', query_heads, key_heads) / math.sqrt(HEAD_DIM)
    positions = jnp.arange(seq_len, dtype=jnp.int32)
    scores = jnp.where(positions[:, None] >= positions[None, :], scores, -1e+30)
    softmax_weights = jax.nn.softmax(scores, axis=-1).astype(jnp.bfloat16)
    heads_out = jnp.einsum('gjts,sgd->tgjd', softmax_weights.astype(jnp.float32), value_heads)
    heads_out = heads_out.astype(jnp.bfloat16).reshape(seq_len, HEADS * HEAD_DIM)
    grouped = heads_out.astype(jnp.float32).reshape(seq_len, N_TENSOR, -1)
    grouped_weight = output_part.astype(jnp.float32).reshape(N_TENSOR, -1, D)
    partials = jnp.einsum('tnc,ncd->ntd', grouped, grouped_weight)
    partials = lax.optimization_barrier(partials.astype(jnp.bfloat16)).astype(jnp.float32)
    attention_sum = lax.optimization_barrier(jnp.sum(partials, axis=0))
    return (token_rows.astype(jnp.float32) + attention_sum).astype(jnp.bfloat16)

def reference(section_input, history, query_weight, key_weight, value_weight, output_weight, mix_weights):
    block_outs = lax.map(one_section, (section_input, query_weight, key_weight, value_weight, output_weight))
    section_numbers = jnp.arange(N_SECTION, dtype=jnp.int32)
    mixed_sum = mix_weights[:, 0][:, None, None] * block_outs.astype(jnp.float32)
    for history_slot in range(1, HIST + 1):
        sender_section = section_numbers - DILATION_STRIDE * history_slot
        picked = jnp.take(history[:, history_slot - 1], jnp.maximum(sender_section, 0).astype(jnp.int32), axis=0)
        factor = jnp.where(sender_section >= 0, mix_weights[:, history_slot], jnp.float32(0.0))
        mixed_sum = mixed_sum + factor[:, None, None] * picked.astype(jnp.float32)
    mixed = mixed_sum.astype(jnp.bfloat16)
    return jnp.concatenate([mixed[-1:], mixed[:-1]], axis=0)
```

```python
import functools
import math

import jax
import jax.numpy as jnp
from jax import lax
from jax.experimental import pallas as pl
from jax.experimental.pallas import tpu as pltpu
from jax.sharding import PartitionSpec as P

HEAD_DIM = 64
DILATION_STRIDE = 4
MESH = pl.DeviceIdType.MESH
PIECES = 4


def start(copy):
    copy.start()
    return copy


def tick_kernel(
    sections,
    x_hbm,
    hist_hbm,
    wq_hbm,
    wk_hbm,
    wv_hbm,
    wo_hbm,
    mix_hbm,
    out_hbm,
    x_own,
    rows_all,
    w_all,
    w_out,
    q_all,
    k_pad,
    v_pad,
    heads,
    far_send,
    relay_in,
    near_send,
    final_in,
    own_part,
    mixed,
    block_in,
    hist_in,
    mix_v,
    w_sem,
    wo_sem,
    x_sem,
    mix_sem,
    hist_s,
    hist_r,
    ag_s,
    ag_r,
    fw_s,
    fw_r,
    far_s,
    far_r,
    near_s,
    near_r,
    out_s,
    out_r,
    store_sem,
):
    section = lax.axis_index("section")
    me = lax.axis_index("tensor")
    right, left, far = lax.rem(me + 1, 4), lax.rem(me + 3, 4), lax.rem(me + 2, 4)
    to = (right, left)
    source = (left, right)
    rows, width = x_own.shape
    slots = hist_in.shape[0]
    piece = rows // PIECES
    q_tiles = w_all.shape[0] - 1
    tile = w_all.shape[2]
    half = tile // 2
    col_chunks, _, cols = w_out.shape
    side = col_chunks // 2
    nxt = lax.rem(section + 1, sections)
    prv = lax.rem(section + sections - 1, sections)

    load_x = start(pltpu.make_async_copy(x_hbm.at[0], x_own, x_sem))
    barrier = pltpu.get_barrier_semaphore()
    for other in to:
        pl.semaphore_signal(barrier, inc=1, device_id={"tensor": other}, device_id_type=MESH)
    for other in (nxt, prv):
        pl.semaphore_signal(barrier, inc=1, device_id={"section": other}, device_id_type=MESH)
    expected = jnp.int32(4)
    for k in range(1, slots + 1):
        step = DILATION_STRIDE * k
        forward, backward = section + step < sections, prv >= step

        @pl.when(forward)
        def _():
            pl.semaphore_signal(
                barrier,
                inc=1,
                device_id={"section": lax.rem(section + step + 1, sections)},
                device_id_type=MESH,
            )

        @pl.when(backward)
        def _():
            pl.semaphore_signal(
                barrier, inc=1, device_id={"section": prv - step}, device_id_type=MESH
            )

        expected = expected + forward.astype(jnp.int32) + backward.astype(jnp.int32)

    loads = []
    for j in range(q_tiles):
        loads.append(
            pltpu.make_async_copy(
                wq_hbm.at[0, :, pl.ds(j * tile, tile)], w_all.at[j], w_sem.at[j]
            )
        )
    loads.append(
        pltpu.make_async_copy(
            wk_hbm.at[0], w_all.at[q_tiles, :, pl.ds(0, half)], w_sem.at[q_tiles]
        )
    )
    loads.append(
        pltpu.make_async_copy(
            wv_hbm.at[0], w_all.at[q_tiles, :, pl.ds(half, half)], w_sem.at[q_tiles + 1]
        )
    )
    load_x.wait()
    for copy in loads:
        copy.start()
    load_mix = start(pltpu.make_async_copy(mix_hbm, mix_v, mix_sem))

    def norm_rows(i, carry):
        at = pl.multiple_of(i * 16, 16)
        values = x_own[pl.ds(at, 16), :].astype(jnp.float32)
        inv = lax.rsqrt(jnp.mean(values * values, axis=-1, keepdims=True) + 1e-05)
        rows_all[me, pl.ds(at, 16), :] = (values * inv).astype(jnp.bfloat16)
        return carry

    lax.fori_loop(0, rows // 16, norm_rows, 0)
    pl.semaphore_wait(barrier, expected)

    def own_copy(way, p):
        place = rows_all.at[me, pl.ds(p * piece, piece)]
        return pltpu.make_async_remote_copy(
            src_ref=place,
            dst_ref=place,
            send_sem=ag_s.at[way, p],
            recv_sem=ag_r.at[way, p],
            device_id={"tensor": to[way]},
            device_id_type=MESH,
        )

    def pass_copy(p):
        way = 0 if p < PIECES // 2 else 1
        place = rows_all.at[source[way], pl.ds(p * piece, piece)]
        return pltpu.make_async_remote_copy(
            src_ref=place,
            dst_ref=place,
            send_sem=fw_s.at[p],
            recv_sem=fw_r.at[p],
            device_id={"tensor": to[way]},
            device_id_type=MESH,
        )

    for p in range(PIECES):
        own_copy(0, p).start()
        own_copy(1, PIECES - 1 - p).start()

    def hist_copy(k):
        return pltpu.make_async_remote_copy(
            src_ref=hist_hbm.at[0, k - 1],
            dst_ref=hist_in.at[k - 1],
            send_sem=hist_s.at[k - 1],
            recv_sem=hist_r.at[k - 1],
            device_id={"section": lax.rem(section + DILATION_STRIDE * k + 1, sections)},
            device_id_type=MESH,
        )

    for k in range(1, slots + 1):
        step = DILATION_STRIDE * k

        @pl.when(section + step < sections)
        def _():
            hist_copy(k).start()

        @pl.when(prv < step)
        def _():
            hist_in[k - 1] = jnp.zeros((rows, width), hist_in.dtype)

    out_loads = []
    for c in range(col_chunks):
        out_loads.append(
            start(
                pltpu.make_async_copy(
                    wo_hbm.at[0, :, pl.ds(c * cols, cols)], w_out.at[c], wo_sem.at[c]
                )
            )
        )

    scale = 1.0 / math.sqrt(HEAD_DIM)

    def project(block):
        where = pl.ds(pl.multiple_of(block * rows, rows), rows)

        def q_tile(j, carry):
            acc = jnp.dot(rows_all[block], w_all[j], preferred_element_type=jnp.float32)
            acc = acc.astype(jnp.bfloat16) * jnp.bfloat16(scale)
            q_all[2 * j, where, :] = acc[:, :half]
            q_all[2 * j + 1, where, :] = acc[:, half:]
            return carry

        lax.fori_loop(0, q_tiles, q_tile, 0)
        acc = jnp.dot(rows_all[block], w_all[q_tiles], preferred_element_type=jnp.float32)
        acc = acc.astype(jnp.bfloat16).astype(jnp.float32)
        for part, padded in ((acc[:, :half], k_pad), (acc[:, half:], v_pad)):
            lane = lax.broadcasted_iota(jnp.int32, part.shape, 1)
            turned = pltpu.roll(part, HEAD_DIM, 1)
            low = lane < HEAD_DIM
            zero = jnp.zeros_like(part)
            forms = (
                jnp.where(low, part, zero),
                jnp.where(low, zero, turned),
                jnp.where(low, turned, zero),
                jnp.where(low, zero, part),
            )
            for f, form in enumerate(forms):
                padded[f, where, :] = form.astype(jnp.bfloat16)

    pairs = q_all.shape[0]
    pairs_per_kv = pairs // (half // HEAD_DIM)

    def attend(block, wanted):
        for b in range(4):
            keys = (b + 1) * rows

            @pl.when(wanted & (block == b))
            def _():
                def pair(p, carry):
                    query = q_all[p, b * rows : (b + 1) * rows, :]
                    row_at = b * rows + lax.broadcasted_iota(jnp.int32, (rows, keys), 0)
                    key_at = lax.broadcasted_iota(jnp.int32, (rows, keys), 1)
                    seen = row_at >= key_at
                    kv = p // pairs_per_kv
                    total = None
                    for which in range(2):
                        scores = lax.dot_general(
                            query,
                            k_pad[kv * 2 + which, :keys, :],
                            (((1,), (1,)), ((), ())),
                            preferred_element_type=jnp.float32,
                        )
                        scores = jnp.where(seen, scores, -1e30)
                        top = jnp.max(scores, axis=-1, keepdims=True)
                        weights = jnp.exp(scores - top)
                        weights = weights * (1.0 / jnp.sum(weights, axis=-1, keepdims=True))
                        term = jnp.dot(
                            weights.astype(jnp.bfloat16),
                            v_pad[kv * 2 + which, :keys, :],
                            preferred_element_type=jnp.float32,
                        )
                        total = term if total is None else total + term
                    heads[b, :, pl.ds(pl.multiple_of(p * half, half), half)] = total.astype(
                        jnp.bfloat16
                    )
                    return carry

                lax.fori_loop(0, pairs, pair, 0)

    def part(block, c):
        acc = jnp.dot(heads[block], w_out[c], preferred_element_type=jnp.float32)
        return acc.astype(jnp.bfloat16)

    def far_copy(c, way):
        return pltpu.make_async_remote_copy(
            src_ref=far_send.at[c],
            dst_ref=relay_in.at[c],
            send_sem=far_s.at[c],
            recv_sem=far_r.at[c],
            device_id={"tensor": to[way]},
            device_id_type=MESH,
        )

    def near_copy(way, c):
        return pltpu.make_async_remote_copy(
            src_ref=near_send.at[way, c],
            dst_ref=final_in.at[way, c],
            send_sem=near_s.at[way, c],
            recv_sem=near_r.at[way, c],
            device_id={"tensor": to[way]},
            device_id_type=MESH,
        )

    def out_copy(c):
        return pltpu.make_async_remote_copy(
            src_ref=mixed.at[c],
            dst_ref=block_in.at[c],
            send_sem=out_s.at[c],
            recv_sem=out_r.at[c],
            device_id={"section": nxt},
            device_id_type=MESH,
        )

    for copy in loads:
        copy.wait()
    project(me)

    def arrived(way, p):
        place = rows_all.at[source[way], pl.ds(p * piece, piece)]
        return pltpu.make_async_remote_copy(
            src_ref=place,
            dst_ref=place,
            send_sem=ag_s.at[way, p],
            recv_sem=ag_r.at[way, p],
            device_id={"tensor": to[way]},
            device_id_type=MESH,
        )

    def far_arrived(p):
        place = rows_all.at[far, pl.ds(p * piece, piece)]
        return pltpu.make_async_remote_copy(
            src_ref=place,
            dst_ref=place,
            send_sem=fw_s.at[p],
            recv_sem=fw_r.at[p],
            device_id={"tensor": right},
            device_id_type=MESH,
        )

    for p in range(PIECES // 2):
        q = PIECES - 1 - p
        arrived(0, p).wait_recv()
        pass_copy(p).start()
        arrived(1, q).wait_recv()
        pass_copy(q).start()
    for copy in out_loads:
        copy.wait()
    load_mix.wait()
    for p in range(PIECES // 2):
        arrived(0, PIECES - 1 - p).wait_recv()
        arrived(1, p).wait_recv()
    for near in (left, right):
        project(near)
    attend(me, far > me)

    for p in range(PIECES):
        far_arrived(p).wait_recv()
    project(far)
    attend(far, True)

    def far_step(i, carry):
        far_send[i] = part(far, i)
        far_copy(i, 1).start()
        far_send[side + i] = part(far, side + i)
        far_copy(side + i, 0).start()
        return carry

    lax.fori_loop(0, side, far_step, 0)

    attend(right, True)
    attend(left, True)

    def near_step(i, carry):
        for way in range(2):
            relay = side + i if way == 0 else i
            direct = i if way == 0 else side + i
            value = part(to[way], relay)
            far_copy(relay, way).wait_recv()
            total = value.astype(jnp.float32) + relay_in[relay].astype(jnp.float32)
            near_send[way, relay] = total.astype(jnp.bfloat16)
            near_copy(way, relay).start()
            near_send[way, direct] = part(to[way], direct)
            near_copy(way, direct).start()
        return carry

    lax.fori_loop(0, side, near_step, 0)
    attend(me, far < me)

    def own_step(c, carry):
        own_part[c] = part(me, c)
        return carry

    lax.fori_loop(0, col_chunks, own_step, 0)

    def column(i):
        return (i % 2) * side + i // 2

    def final_step(i, carry):
        c = column(i)
        where = pl.ds(pl.multiple_of(c * cols, cols), cols)
        total = own_part[c].astype(jnp.float32)
        for way in range(2):
            near_copy(way, c).wait_recv()
            total = total + final_in[way, c].astype(jnp.float32)
        block = (x_own[:, where].astype(jnp.float32) + total).astype(jnp.bfloat16)
        mixed[c] = block
        out_copy(c).start()
        return carry

    lax.fori_loop(0, col_chunks, final_step, 0)

    for k in range(1, slots + 1):

        @pl.when(prv >= DILATION_STRIDE * k)
        def _():
            hist_copy(k).wait_recv()

    def store_copy(c):
        return pltpu.make_async_copy(
            block_in.at[c],
            out_hbm.at[0, :, pl.ds(pl.multiple_of(c * cols, cols), cols)],
            store_sem.at[c],
        )

    def mix_step(i, carry):
        c = column(i)
        out_copy(c).wait_recv()
        where = pl.ds(pl.multiple_of(c * cols, cols), cols)
        factors = mix_v[pl.ds(prv, 1), :]
        value = factors[:, 0:1] * block_in[c].astype(jnp.float32)
        for k in range(1, slots + 1):
            past = hist_in[k - 1, :, where].astype(jnp.float32)
            value = value + factors[:, k : k + 1] * past
        block_in[c] = value.astype(jnp.bfloat16)
        store_copy(c).start()
        return carry

    lax.fori_loop(0, col_chunks, mix_step, 0)

    for p in range(PIECES):
        own_copy(0, p).wait_send()
        own_copy(1, p).wait_send()
        pass_copy(p).wait_send()
    for k in range(1, slots + 1):

        @pl.when(section + DILATION_STRIDE * k < sections)
        def _():
            hist_copy(k).wait_send()

    def drain(c, carry):
        far_copy(c, 0).wait_send()
        near_copy(0, c).wait_send()
        near_copy(1, c).wait_send()
        out_copy(c).wait_send()
        store_copy(c).wait()
        return carry

    lax.fori_loop(0, col_chunks, drain, 0)


def solution(mesh):
    sections, tensor = mesh.shape["section"], mesh.shape["tensor"]
    assert tensor == 4
    col_chunks = 8

    def on_device(x, history, wq, wk, wv, wo, mix_weights):
        rows, width = x.shape[1:]
        slots = history.shape[1]
        q_width, kv_width = wq.shape[2], wk.shape[2]
        seq = rows * tensor
        tile = 2 * kv_width
        q_tiles = q_width // tile
        cols = width // col_chunks
        bf16 = jnp.bfloat16
        dma = pltpu.SemaphoreType.DMA
        hbm = pl.BlockSpec(memory_space=pl.ANY)
        return pl.pallas_call(
            functools.partial(tick_kernel, sections),
            out_shape=jax.ShapeDtypeStruct(x.shape, bf16),
            in_specs=[hbm] * 7,
            out_specs=hbm,
            scratch_shapes=[
                pltpu.VMEM((rows, width), bf16),
                pltpu.VMEM((tensor, rows, width), bf16),
                pltpu.VMEM((q_tiles + 1, width, tile), bf16),
                pltpu.VMEM((col_chunks, q_width, cols), bf16),
                pltpu.VMEM((2 * q_tiles, seq, kv_width), bf16),
                pltpu.VMEM((4, seq, kv_width), bf16),
                pltpu.VMEM((4, seq, kv_width), bf16),
                pltpu.VMEM((tensor, rows, q_width), bf16),
                pltpu.VMEM((col_chunks, rows, cols), bf16),
                pltpu.VMEM((col_chunks, rows, cols), bf16),
                pltpu.VMEM((2, col_chunks, rows, cols), bf16),
                pltpu.VMEM((2, col_chunks, rows, cols), bf16),
                pltpu.VMEM((col_chunks, rows, cols), bf16),
                pltpu.VMEM((col_chunks, rows, cols), bf16),
                pltpu.VMEM((col_chunks, rows, cols), bf16),
                pltpu.VMEM((slots, rows, width), bf16),
                pltpu.VMEM(mix_weights.shape, mix_weights.dtype),
                dma((q_tiles + 2,)),
                dma((col_chunks,)),
                dma,
                dma,
                dma((slots,)),
                dma((slots,)),
                dma((2, PIECES)),
                dma((2, PIECES)),
                dma((PIECES,)),
                dma((PIECES,)),
                dma((col_chunks,)),
                dma((col_chunks,)),
                dma((2, col_chunks)),
                dma((2, col_chunks)),
                dma((col_chunks,)),
                dma((col_chunks,)),
                dma((col_chunks,)),
            ],
            compiler_params=pltpu.CompilerParams(
                collective_id=0, has_side_effects=True, vmem_limit_bytes=60 * 1024 * 1024
            ),
        )(x, history, wq, wk, wv, wo, mix_weights)

    placed = (
        P("section", "tensor", None),
        P("section", None, "tensor", None),
        P("section", None, "tensor"),
        P("section", None, "tensor"),
        P("section", None, "tensor"),
        P("section", "tensor", None),
        P(),
    )
    return jax.shard_map(
        on_device,
        mesh=mesh,
        in_specs=placed,
        out_specs=P("section", "tensor", None),
        check_vma=False,
    )
```

```python
import functools
import math

import jax
import jax.numpy as jnp
from jax import lax
from jax.experimental import pallas as pl
from jax.experimental.pallas import tpu as pltpu
from jax.sharding import PartitionSpec as P

HEAD_DIM = 64
WIDE_CHUNKS = 5
MESH = pl.DeviceIdType.MESH
PIECES = 4


def start(copy):
    copy.start()
    return copy


def tick_kernel(
    sections,
    x_hbm,
    hist_hbm,
    wq_hbm,
    wk_hbm,
    wv_hbm,
    wo_hbm,
    mix_hbm,
    out_hbm,
    x_own,
    rows_all,
    w_all,
    w_out,
    q_all,
    k_pad,
    v_pad,
    heads,
    far_send,
    relay_in,
    near_send,
    final_in,
    own_part,
    mixed,
    even,
    cross_in,
    part_out,
    part_in,
    raw_a,
    raw_b,
    first,
    pair_out,
    pair_in,
    past,
    mix_v,
    w_sem,
    wo_sem,
    x_sem,
    mix_sem,
    even_sem,
    first_sem,
    cross_s,
    cross_r,
    part_s,
    part_r,
    raw_s,
    raw_r,
    pair_s,
    pair_r,
    ag_s,
    ag_r,
    fw_s,
    fw_r,
    far_s,
    far_r,
    near_s,
    near_r,
    out_s,
    out_r,
):
    section = lax.axis_index("section")
    me = lax.axis_index("tensor")
    right, left, far = lax.rem(me + 1, 4), lax.rem(me + 3, 4), lax.rem(me + 2, 4)
    to = (right, left)
    source = (left, right)
    rows, width = x_own.shape
    piece = rows // PIECES
    q_tiles = w_all.shape[0] - 1
    tile = w_all.shape[2]
    half = tile // 2
    col_chunks, _, cols = w_out.shape
    side = col_chunks // 2
    nxt = lax.rem(section + 1, sections)
    prv = lax.rem(section + sections - 1, sections)

    load_x = start(pltpu.make_async_copy(x_hbm.at[0], x_own, x_sem))
    barrier = pltpu.get_barrier_semaphore()
    for other in to:
        pl.semaphore_signal(barrier, inc=1, device_id={"tensor": other}, device_id_type=MESH)
    row, col = section // 8, lax.rem(section // 4, 2)
    partner = section + 4 - 8 * col
    others = [lax.rem(section + 8 * d, sections) for d in (1, 2, 3)]
    for other in (nxt, prv, partner, *others):
        pl.semaphore_signal(barrier, inc=1, device_id={"section": other}, device_id_type=MESH)

    loads = []
    for j in range(q_tiles):
        loads.append(
            pltpu.make_async_copy(
                wq_hbm.at[0, :, pl.ds(j * tile, tile)], w_all.at[j], w_sem.at[j]
            )
        )
    loads.append(
        pltpu.make_async_copy(
            wk_hbm.at[0], w_all.at[q_tiles, :, pl.ds(0, half)], w_sem.at[q_tiles]
        )
    )
    loads.append(
        pltpu.make_async_copy(
            wv_hbm.at[0], w_all.at[q_tiles, :, pl.ds(half, half)], w_sem.at[q_tiles + 1]
        )
    )
    load_x.wait()
    for copy in loads:
        copy.start()
    load_mix = start(pltpu.make_async_copy(mix_hbm, mix_v, mix_sem))

    def norm_rows(i, carry):
        at = pl.multiple_of(i * 16, 16)
        values = x_own[pl.ds(at, 16), :].astype(jnp.float32)
        inv = lax.rsqrt(jnp.mean(values * values, axis=-1, keepdims=True) + 1e-05)
        rows_all[me, pl.ds(at, 16), :] = (values * inv).astype(jnp.bfloat16)
        return carry

    lax.fori_loop(0, rows // 16, norm_rows, 0)
    pl.semaphore_wait(barrier, 8)

    def own_copy(way, p):
        place = rows_all.at[me, pl.ds(p * piece, piece)]
        return pltpu.make_async_remote_copy(
            src_ref=place,
            dst_ref=place,
            send_sem=ag_s.at[way, p],
            recv_sem=ag_r.at[way, p],
            device_id={"tensor": to[way]},
            device_id_type=MESH,
        )

    def pass_copy(p):
        way = 0 if p < PIECES // 2 else 1
        place = rows_all.at[source[way], pl.ds(p * piece, piece)]
        return pltpu.make_async_remote_copy(
            src_ref=place,
            dst_ref=place,
            send_sem=fw_s.at[p],
            recv_sem=fw_r.at[p],
            device_id={"tensor": to[way]},
            device_id_type=MESH,
        )

    for p in range(PIECES):
        own_copy(0, p).start()
        own_copy(1, PIECES - 1 - p).start()

    wide = even.shape[2]
    wide_chunks = wide // cols
    narrow_chunks = col_chunks - wide_chunks
    lead, tail = pl.ds(0, wide), pl.ds(wide, width - wide)
    steps = range(1, 4)

    def onward(d):
        return row + d < 4

    def inward(d):
        return row >= d

    def cross_sent(d):
        return onward(d) if d else col == 0

    def cross_due(d):
        return onward(d) if d else col == 1

    def section_copy(src, dst, send, recv, target):
        return pltpu.make_async_remote_copy(
            src_ref=src,
            dst_ref=dst,
            send_sem=send,
            recv_sem=recv,
            device_id={"section": target},
            device_id_type=MESH,
        )

    def cross_copy(d):
        return section_copy(
            hist_hbm.at[0, jnp.maximum(2 * d - 2 * col, 0), :, lead],
            cross_in.at[d],
            cross_s.at[d],
            cross_r.at[d],
            partner,
        )

    def part_copy(d):
        return section_copy(
            part_out.at[d - 1], part_in.at[d - 1], part_s.at[d - 1], part_r.at[d - 1], others[d - 1]
        )

    def raw_copy(d, which):
        slot = 2 * d - 1 if which == 0 else 2 * d - 2 * col
        return section_copy(
            hist_hbm.at[0, slot, :, tail],
            (raw_a, raw_b)[which].at[d - 1],
            raw_s.at[which, d - 1],
            raw_r.at[which, d - 1],
            others[d - 1],
        )

    def pair_copy():
        return section_copy(pair_out, pair_in, pair_s, pair_r, partner)

    pair_sent = (row >= 1) | (col == 0)
    pair_due = (row >= 1) | (col == 1)

    def even_load(d):
        return pltpu.make_async_copy(
            hist_hbm.at[0, 2 * d - 1, :, lead], even.at[d - 1], even_sem.at[d - 1]
        )

    first_load = pltpu.make_async_copy(hist_hbm.at[0, 0, :, tail], first, first_sem)

    for d in (1, 2, 3, 0):

        @pl.when(cross_sent(d))
        def _():
            cross_copy(d).start()

    for d in steps:

        @pl.when(onward(d))
        def _():
            raw_copy(d, 1).start()
            raw_copy(d, 0).start()

    out_loads = []
    for c in range(col_chunks):
        out_loads.append(
            start(
                pltpu.make_async_copy(
                    wo_hbm.at[0, :, pl.ds(c * cols, cols)], w_out.at[c], wo_sem.at[c]
                )
            )
        )

    for d in steps:

        @pl.when(onward(d))
        def _():
            even_load(d).start()

        @pl.when(row < d)
        def _():
            part_in[d - 1] = jnp.zeros(part_in.shape[1:], part_in.dtype)
            raw_a[d - 1] = jnp.zeros(raw_a.shape[1:], raw_a.dtype)
            raw_b[d - 1] = jnp.zeros(raw_b.shape[1:], raw_b.dtype)

    @pl.when(col == 0)
    def _():
        first_load.start()
        cross_in[0] = jnp.zeros(cross_in.shape[1:], cross_in.dtype)

    @pl.when(col == 1)
    def _():
        first[...] = jnp.zeros(first.shape, first.dtype)

    @pl.when(jnp.logical_not(pair_due))
    def _():
        pair_in[...] = jnp.zeros(pair_in.shape, pair_in.dtype)

    def weight(target, k):
        table = mix_v[...]
        at = (lax.broadcasted_iota(jnp.int32, table.shape, 0) == k) & (
            lax.broadcasted_iota(jnp.int32, table.shape, 1) == target
        )
        return jnp.sum(jnp.where(at, table, 0.0), keepdims=True)

    def chunk(c):
        return pl.ds(pl.multiple_of(c * cols, cols), cols)

    def relay(d):
        @pl.when(onward(d))
        def _():
            with jax.named_scope(f"relay{d}"):
                own_weight = weight(section + 8 * d, 2 * d)
                partner_weight = weight(section + 8 * d, 2 * d - 1 + 2 * col)
                even_load(d).wait()
                cross_copy(d).wait_recv()

                def add(c, carry):
                    at = chunk(c)
                    value = own_weight * even[d - 1, :, at].astype(jnp.float32)
                    value = value + partner_weight * cross_in[d, :, at].astype(jnp.float32)
                    part_out[d - 1, :, at] = value.astype(jnp.bfloat16)
                    return carry

                lax.fori_loop(0, wide_chunks, add, 0)
                part_copy(d).start()

    def relay_pair():
        @pl.when(col == 0)
        def _():
            first_load.wait()

        for d in steps:

            @pl.when(inward(d))
            def _():
                raw_copy(d, 1).wait_recv()

        @pl.when(pair_sent)
        def _():
            weights = [weight(partner, 2 * d + 1 - 2 * col) for d in steps]
            first_weight = weight(partner, 1)

            def add(c, carry):
                at = chunk(c)
                value = first_weight * first[:, at].astype(jnp.float32)
                for d in steps:
                    value = value + weights[d - 1] * raw_b[d - 1, :, at].astype(jnp.float32)
                pair_out[:, at] = value.astype(jnp.bfloat16)
                return carry

            lax.fori_loop(0, narrow_chunks, add, 0)
            pair_copy().start()

    def gather_past():
        @pl.when(col == 1)
        def _():
            cross_copy(0).wait_recv()

        for d in steps:

            @pl.when(inward(d))
            def _():
                part_copy(d).wait_recv()
                raw_copy(d, 0).wait_recv()

        @pl.when(pair_due)
        def _():
            pair_copy().wait_recv()

        cross_weight = weight(section, 1)

        def add_wide(c, carry):
            at = chunk(c)
            value = cross_weight * cross_in[0, :, at].astype(jnp.float32)
            for d in steps:
                value = value + part_in[d - 1, :, at].astype(jnp.float32)
            past[c] = value
            return carry

        lax.fori_loop(0, wide_chunks, add_wide, 0)
        weights = [weight(section, 2 * d) for d in steps]

        def add_narrow(c, carry):
            at = chunk(c)
            value = pair_in[:, at].astype(jnp.float32)
            for d in steps:
                value = value + weights[d - 1] * raw_a[d - 1, :, at].astype(jnp.float32)
            past[wide_chunks + c] = value
            return carry

        lax.fori_loop(0, narrow_chunks, add_narrow, 0)

    scale = 1.0 / math.sqrt(HEAD_DIM)

    def project(block):
        where = pl.ds(pl.multiple_of(block * rows, rows), rows)

        def q_tile(j, carry):
            acc = jnp.dot(rows_all[block], w_all[j], preferred_element_type=jnp.float32)
            acc = acc.astype(jnp.bfloat16) * jnp.bfloat16(scale)
            q_all[2 * j, where, :] = acc[:, :half]
            q_all[2 * j + 1, where, :] = acc[:, half:]
            return carry

        lax.fori_loop(0, q_tiles, q_tile, 0)
        acc = jnp.dot(rows_all[block], w_all[q_tiles], preferred_element_type=jnp.float32)
        acc = acc.astype(jnp.bfloat16).astype(jnp.float32)
        for part, padded in ((acc[:, :half], k_pad), (acc[:, half:], v_pad)):
            lane = lax.broadcasted_iota(jnp.int32, part.shape, 1)
            turned = pltpu.roll(part, HEAD_DIM, 1)
            low = lane < HEAD_DIM
            zero = jnp.zeros_like(part)
            forms = (
                jnp.where(low, part, zero),
                jnp.where(low, zero, turned),
                jnp.where(low, turned, zero),
                jnp.where(low, zero, part),
            )
            for f, form in enumerate(forms):
                padded[f, where, :] = form.astype(jnp.bfloat16)

    pairs = q_all.shape[0]
    pairs_per_kv = pairs // (half // HEAD_DIM)

    def attend(block, wanted):
        for b in range(4):
            keys = (b + 1) * rows

            @pl.when(wanted & (block == b))
            def _():
                def pair(p, carry):
                    query = q_all[p, b * rows : (b + 1) * rows, :]
                    row_at = b * rows + lax.broadcasted_iota(jnp.int32, (rows, keys), 0)
                    key_at = lax.broadcasted_iota(jnp.int32, (rows, keys), 1)
                    seen = row_at >= key_at
                    kv = p // pairs_per_kv
                    total = None
                    for which in range(2):
                        scores = lax.dot_general(
                            query,
                            k_pad[kv * 2 + which, :keys, :],
                            (((1,), (1,)), ((), ())),
                            preferred_element_type=jnp.float32,
                        )
                        scores = jnp.where(seen, scores, -1e30)
                        top = jnp.max(scores, axis=-1, keepdims=True)
                        weights = jnp.exp(scores - top)
                        weights = weights * (1.0 / jnp.sum(weights, axis=-1, keepdims=True))
                        term = jnp.dot(
                            weights.astype(jnp.bfloat16),
                            v_pad[kv * 2 + which, :keys, :],
                            preferred_element_type=jnp.float32,
                        )
                        total = term if total is None else total + term
                    heads[b, :, pl.ds(pl.multiple_of(p * half, half), half)] = total.astype(
                        jnp.bfloat16
                    )
                    return carry

                lax.fori_loop(0, pairs, pair, 0)

    def part(block, c):
        acc = jnp.dot(heads[block], w_out[c], preferred_element_type=jnp.float32)
        return acc.astype(jnp.bfloat16)

    def far_copy(c, way):
        return pltpu.make_async_remote_copy(
            src_ref=far_send.at[c],
            dst_ref=relay_in.at[c],
            send_sem=far_s.at[c],
            recv_sem=far_r.at[c],
            device_id={"tensor": to[way]},
            device_id_type=MESH,
        )

    def near_copy(way, c):
        return pltpu.make_async_remote_copy(
            src_ref=near_send.at[way, c],
            dst_ref=final_in.at[way, c],
            send_sem=near_s.at[way, c],
            recv_sem=near_r.at[way, c],
            device_id={"tensor": to[way]},
            device_id_type=MESH,
        )

    def out_copy(c):
        return pltpu.make_async_remote_copy(
            src_ref=mixed.at[c],
            dst_ref=out_hbm.at[0, :, pl.ds(pl.multiple_of(c * cols, cols), cols)],
            send_sem=out_s.at[c],
            recv_sem=out_r.at[c],
            device_id={"section": nxt},
            device_id_type=MESH,
        )

    for copy in loads:
        copy.wait()
    project(me)

    def arrived(way, p):
        place = rows_all.at[source[way], pl.ds(p * piece, piece)]
        return pltpu.make_async_remote_copy(
            src_ref=place,
            dst_ref=place,
            send_sem=ag_s.at[way, p],
            recv_sem=ag_r.at[way, p],
            device_id={"tensor": to[way]},
            device_id_type=MESH,
        )

    def far_arrived(p):
        place = rows_all.at[far, pl.ds(p * piece, piece)]
        return pltpu.make_async_remote_copy(
            src_ref=place,
            dst_ref=place,
            send_sem=fw_s.at[p],
            recv_sem=fw_r.at[p],
            device_id={"tensor": right},
            device_id_type=MESH,
        )

    for p in range(PIECES // 2):
        q = PIECES - 1 - p
        arrived(0, p).wait_recv()
        pass_copy(p).start()
        arrived(1, q).wait_recv()
        pass_copy(q).start()
    for copy in out_loads:
        copy.wait()
    load_mix.wait()
    with jax.named_scope("relays"):
        relay(1)
    for p in range(PIECES // 2):
        arrived(0, PIECES - 1 - p).wait_recv()
        arrived(1, p).wait_recv()
    for near in (left, right):
        project(near)
    attend(me, far > me)
    relay(2)

    for p in range(PIECES):
        far_arrived(p).wait_recv()
    project(far)
    attend(far, True)

    def far_step(i, carry):
        far_send[i] = part(far, i)
        far_copy(i, 1).start()
        far_send[side + i] = part(far, side + i)
        far_copy(side + i, 0).start()
        return carry

    lax.fori_loop(0, side, far_step, 0)
    relay(3)
    with jax.named_scope("relay_pair"):
        relay_pair()

    attend(right, True)
    attend(left, True)

    def near_step(i, carry):
        for way in range(2):
            relay = side + i if way == 0 else i
            direct = i if way == 0 else side + i
            value = part(to[way], relay)
            far_copy(relay, way).wait_recv()
            total = value.astype(jnp.float32) + relay_in[relay].astype(jnp.float32)
            near_send[way, relay] = total.astype(jnp.bfloat16)
            near_copy(way, relay).start()
            near_send[way, direct] = part(to[way], direct)
            near_copy(way, direct).start()
        return carry

    lax.fori_loop(0, side, near_step, 0)
    attend(me, far < me)

    def own_step(c, carry):
        own_part[c] = part(me, c)
        return carry

    lax.fori_loop(0, col_chunks, own_step, 0)

    with jax.named_scope("past"):
        gather_past()
    own_weight = weight(section, 0)

    def column(i):
        return (i % 2) * side + i // 2

    def final_step(i, carry):
        c = column(i)
        where = pl.ds(pl.multiple_of(c * cols, cols), cols)
        total = own_part[c].astype(jnp.float32)
        for way in range(2):
            near_copy(way, c).wait_recv()
            total = total + final_in[way, c].astype(jnp.float32)
        block = (x_own[:, where].astype(jnp.float32) + total).astype(jnp.bfloat16)
        mixed[c] = (own_weight * block.astype(jnp.float32) + past[c]).astype(jnp.bfloat16)
        out_copy(c).start()
        return carry

    lax.fori_loop(0, col_chunks, final_step, 0)

    for p in range(PIECES):
        own_copy(0, p).wait_send()
        own_copy(1, p).wait_send()
        pass_copy(p).wait_send()
    for d in (0, *steps):

        @pl.when(cross_sent(d))
        def _():
            cross_copy(d).wait_send()

    for d in steps:

        @pl.when(onward(d))
        def _():
            part_copy(d).wait_send()
            raw_copy(d, 0).wait_send()
            raw_copy(d, 1).wait_send()

    @pl.when(pair_sent)
    def _():
        pair_copy().wait_send()

    def drain(c, carry):
        far_copy(c, 0).wait_send()
        near_copy(0, c).wait_send()
        near_copy(1, c).wait_send()
        out_copy(c).wait()
        return carry

    lax.fori_loop(0, col_chunks, drain, 0)


def solution(mesh):
    sections, tensor = mesh.shape["section"], mesh.shape["tensor"]
    assert tensor == 4 and sections == 32
    col_chunks = 8

    def on_device(x, history, wq, wk, wv, wo, mix_weights):
        rows, width = x.shape[1:]
        q_width, kv_width = wq.shape[2], wk.shape[2]
        seq = rows * tensor
        tile = 2 * kv_width
        q_tiles = q_width // tile
        cols = width // col_chunks
        wide = WIDE_CHUNKS * cols
        bf16 = jnp.bfloat16
        dma = pltpu.SemaphoreType.DMA
        hbm = pl.BlockSpec(memory_space=pl.ANY)
        return pl.pallas_call(
            functools.partial(tick_kernel, sections),
            out_shape=jax.ShapeDtypeStruct(x.shape, bf16),
            in_specs=[hbm] * 7,
            out_specs=hbm,
            scratch_shapes=[
                pltpu.VMEM((rows, width), bf16),
                pltpu.VMEM((tensor, rows, width), bf16),
                pltpu.VMEM((q_tiles + 1, width, tile), bf16),
                pltpu.VMEM((col_chunks, q_width, cols), bf16),
                pltpu.VMEM((2 * q_tiles, seq, kv_width), bf16),
                pltpu.VMEM((4, seq, kv_width), bf16),
                pltpu.VMEM((4, seq, kv_width), bf16),
                pltpu.VMEM((tensor, rows, q_width), bf16),
                pltpu.VMEM((col_chunks, rows, cols), bf16),
                pltpu.VMEM((col_chunks, rows, cols), bf16),
                pltpu.VMEM((2, col_chunks, rows, cols), bf16),
                pltpu.VMEM((2, col_chunks, rows, cols), bf16),
                pltpu.VMEM((col_chunks, rows, cols), bf16),
                pltpu.VMEM((col_chunks, rows, cols), bf16),
                pltpu.VMEM((3, rows, wide), bf16),
                pltpu.VMEM((4, rows, wide), bf16),
                pltpu.VMEM((3, rows, wide), bf16),
                pltpu.VMEM((3, rows, wide), bf16),
                pltpu.VMEM((3, rows, width - wide), bf16),
                pltpu.VMEM((3, rows, width - wide), bf16),
                pltpu.VMEM((rows, width - wide), bf16),
                pltpu.VMEM((rows, width - wide), bf16),
                pltpu.VMEM((rows, width - wide), bf16),
                pltpu.VMEM((col_chunks, rows, cols), jnp.float32),
                pltpu.VMEM(mix_weights.shape[::-1], mix_weights.dtype),
                dma((q_tiles + 2,)),
                dma((col_chunks,)),
                dma,
                dma,
                dma((3,)),
                dma,
                dma((4,)),
                dma((4,)),
                dma((3,)),
                dma((3,)),
                dma((2, 3)),
                dma((2, 3)),
                dma,
                dma,
                dma((2, PIECES)),
                dma((2, PIECES)),
                dma((PIECES,)),
                dma((PIECES,)),
                dma((col_chunks,)),
                dma((col_chunks,)),
                dma((2, col_chunks)),
                dma((2, col_chunks)),
                dma((col_chunks,)),
                dma((col_chunks,)),
            ],
            compiler_params=pltpu.CompilerParams(
                collective_id=0, has_side_effects=True, vmem_limit_bytes=60 * 1024 * 1024
            ),
        )(x, history, wq, wk, wv, wo, mix_weights.T)

    placed = (
        P("section", "tensor", None),
        P("section", None, "tensor", None),
        P("section", None, "tensor"),
        P("section", None, "tensor"),
        P("section", None, "tensor"),
        P("section", "tensor", None),
        P(),
    )
    return jax.shard_map(
        on_device,
        mesh=mesh,
        in_specs=placed,
        out_specs=P("section", "tensor", None),
        check_vma=False,
    )
```

```python
import functools
import math

import jax
import jax.numpy as jnp
from jax import lax
from jax.experimental import pallas as pl
from jax.experimental.pallas import tpu as pltpu
from jax.sharding import PartitionSpec as P

HEAD_DIM = 64
SUMMED = (4, 0, 5, 1, 3)
PLAIN = (6, 2, 7)
MESH = pl.DeviceIdType.MESH
PIECES = 4


def start(copy):
    copy.start()
    return copy


def tick_kernel(
    sections,
    x_hbm,
    hist_hbm,
    wq_hbm,
    wk_hbm,
    wv_hbm,
    wo_hbm,
    mix_hbm,
    out_hbm,
    x_own,
    rows_all,
    w_all,
    w_out,
    q_all,
    k_pad,
    v_pad,
    heads,
    far_send,
    relay_in,
    near_send,
    final_in,
    own_part,
    mixed,
    even,
    cross_in,
    part_out,
    part_in,
    raw_a,
    raw_b,
    first,
    pair_out,
    pair_in,
    past,
    mix_v,
    w_sem,
    wo_sem,
    x_sem,
    mix_sem,
    even_sem,
    first_sem,
    cross_s,
    cross_r,
    part_s,
    part_r,
    raw_s,
    raw_r,
    pair_s,
    pair_r,
    ag_s,
    ag_r,
    fw_s,
    fw_r,
    far_s,
    far_r,
    near_s,
    near_r,
    out_s,
    out_r,
):
    section = lax.axis_index("section")
    me = lax.axis_index("tensor")
    right, left, far = lax.rem(me + 1, 4), lax.rem(me + 3, 4), lax.rem(me + 2, 4)
    to = (right, left)
    source = (left, right)
    rows, width = x_own.shape
    piece = rows // PIECES
    q_tiles = w_all.shape[0] - 1
    tile = w_all.shape[2]
    half = tile // 2
    col_chunks, _, cols = w_out.shape
    side = col_chunks // 2
    nxt = lax.rem(section + 1, sections)
    prv = lax.rem(section + sections - 1, sections)

    def load_x(p):
        at = pl.ds(p * piece, piece)
        return pltpu.make_async_copy(x_hbm.at[0, at], x_own.at[at], x_sem.at[p])

    for p in range(PIECES):
        load_x(p).start()
    barrier = pltpu.get_barrier_semaphore()
    for other in to:
        pl.semaphore_signal(barrier, inc=1, device_id={"tensor": other}, device_id_type=MESH)
    row, col = section // 8, lax.rem(section // 4, 2)
    partner = section + 4 - 8 * col
    others = [lax.rem(section + 8 * d, sections) for d in (1, 2, 3)]
    for other in (nxt, prv, partner, *others):
        pl.semaphore_signal(barrier, inc=1, device_id={"section": other}, device_id_type=MESH)

    loads = []
    for j in range(q_tiles):
        loads.append(
            pltpu.make_async_copy(
                wq_hbm.at[0, :, pl.ds(j * tile, tile)], w_all.at[j], w_sem.at[j]
            )
        )
    loads.append(
        pltpu.make_async_copy(
            wk_hbm.at[0], w_all.at[q_tiles, :, pl.ds(0, half)], w_sem.at[q_tiles]
        )
    )
    loads.append(
        pltpu.make_async_copy(
            wv_hbm.at[0], w_all.at[q_tiles, :, pl.ds(half, half)], w_sem.at[q_tiles + 1]
        )
    )
    load_x(0).wait()
    for copy in loads:
        copy.start()
    load_mix = start(pltpu.make_async_copy(mix_hbm, mix_v, mix_sem))

    def own_copy(way, p):
        place = rows_all.at[me, pl.ds(p * piece, piece)]
        return pltpu.make_async_remote_copy(
            src_ref=place,
            dst_ref=place,
            send_sem=ag_s.at[way],
            recv_sem=ag_r.at[way, p],
            device_id={"tensor": to[way]},
            device_id_type=MESH,
        )

    def settle(ref, send, recv):
        return pltpu.make_async_remote_copy(
            src_ref=ref,
            dst_ref=ref,
            send_sem=send,
            recv_sem=recv,
            device_id={"tensor": right},
            device_id_type=MESH,
        )

    def passed(way, p, block):
        place = rows_all.at[
            block, pl.ds(p * piece, piece), pl.ds(way * (width // 2), width // 2)
        ]
        return pltpu.make_async_remote_copy(
            src_ref=place,
            dst_ref=place,
            send_sem=fw_s.at[way],
            recv_sem=fw_r.at[way, p],
            device_id={"tensor": to[way]},
            device_id_type=MESH,
        )

    def pass_copy(way, p):
        return passed(way, p, source[way])

    def norm_piece(p):
        def norm_rows(i, carry):
            at = pl.ds(pl.multiple_of(p * piece + i * 16, 16), 16)
            values = x_own[at, :].astype(jnp.float32)
            inv = lax.rsqrt(jnp.mean(values * values, axis=-1, keepdims=True) + 1e-05)
            rows_all[me, at, :] = (values * inv).astype(jnp.bfloat16)
            return carry

        lax.fori_loop(0, piece // 16, norm_rows, 0)

    norm_piece(0)
    pl.semaphore_wait(barrier, 8)
    for p in range(PIECES):
        if p:
            load_x(p).wait()
            norm_piece(p)
        own_copy(0, p).start()
        own_copy(1, p).start()

    steps = range(1, 4)

    def chunk(c):
        return pl.ds(c * cols, cols)

    def onward(d):
        return row + d < 4

    def inward(d):
        return row >= d

    def cross_sent(d):
        return onward(d) if d else col == 0

    def cross_due(d):
        return onward(d) if d else col == 1

    def section_copy(src, dst, send, recv, target):
        return pltpu.make_async_remote_copy(
            src_ref=src,
            dst_ref=dst,
            send_sem=send,
            recv_sem=recv,
            device_id={"section": target},
            device_id_type=MESH,
        )

    def cross_copy(d, j):
        return section_copy(
            hist_hbm.at[0, jnp.maximum(2 * d - 2 * col, 0), :, chunk(SUMMED[j])],
            cross_in.at[d, j],
            cross_s.at[d],
            cross_r.at[d, j],
            partner,
        )

    def part_copy(d, j):
        return section_copy(
            part_out.at[d - 1, j],
            part_in.at[d - 1, j],
            part_s.at[d - 1],
            part_r.at[d - 1, j],
            others[d - 1],
        )

    def raw_copy(d, which, n):
        slot = 2 * d - 1 if which == 0 else 2 * d - 2 * col
        return section_copy(
            hist_hbm.at[0, slot, :, chunk(PLAIN[n])],
            (raw_a, raw_b)[which].at[d - 1, n],
            raw_s.at[which, d - 1],
            raw_r.at[which, d - 1],
            others[d - 1],
        )

    def pair_copy(n):
        return section_copy(pair_out.at[n], pair_in.at[n], pair_s, pair_r.at[n], partner)

    pair_sent = (row >= 1) | (col == 0)
    pair_due = (row >= 1) | (col == 1)

    def even_load(d):
        return pltpu.make_async_copy(
            hist_hbm.at[0, 2 * d - 1], even.at[d - 1], even_sem.at[d - 1]
        )

    first_load = pltpu.make_async_copy(hist_hbm.at[0, 0], first, first_sem)

    def cross(some):
        for j in some:
            for d in (1, 2, 3, 0):

                @pl.when(cross_sent(d))
                def _():
                    cross_copy(d, j).start()

    cross(range(len(SUMMED)))

    for which in (1, 0):
        for d in steps:

            @pl.when(onward(d))
            def _():
                for n in range(len(PLAIN)):
                    raw_copy(d, which, n).start()

    out_loads = []
    for c in range(col_chunks):
        out_loads.append(
            start(
                pltpu.make_async_copy(
                    wo_hbm.at[0, :, pl.ds(c * cols, cols)], w_out.at[c], wo_sem.at[c]
                )
            )
        )

    for d in steps:

        @pl.when(onward(d))
        def _():
            even_load(d).start()

        @pl.when(row < d)
        def _():
            part_in[d - 1] = jnp.zeros(part_in.shape[1:], part_in.dtype)
            raw_a[d - 1] = jnp.zeros(raw_a.shape[1:], raw_a.dtype)
            raw_b[d - 1] = jnp.zeros(raw_b.shape[1:], raw_b.dtype)

    @pl.when(col == 0)
    def _():
        first_load.start()
        cross_in[0] = jnp.zeros(cross_in.shape[1:], cross_in.dtype)

    @pl.when(col == 1)
    def _():
        first[...] = jnp.zeros(first.shape, first.dtype)

    @pl.when(jnp.logical_not(pair_due))
    def _():
        pair_in[...] = jnp.zeros(pair_in.shape, pair_in.dtype)

    k_pad[...] = jnp.zeros(k_pad.shape, k_pad.dtype)
    for f in range(v_pad.shape[0]):
        v_pad[f, :, :half] = jnp.zeros((v_pad.shape[1], half), v_pad.dtype)
        v_pad[f, :, half:] = jnp.ones((v_pad.shape[1], half), v_pad.dtype)

    def weight(target, k):
        table = mix_v[...]
        at = (lax.broadcasted_iota(jnp.int32, table.shape, 0) == k) & (
            lax.broadcasted_iota(jnp.int32, table.shape, 1) == target
        )
        return jnp.sum(jnp.where(at, table, 0.0), keepdims=True)

    def relay(j):
        for d in steps:

            @pl.when(onward(d))
            def _():
                own_weight = weight(section + 8 * d, 2 * d)
                partner_weight = weight(section + 8 * d, 2 * d - 1 + 2 * col)
                if j == 0:
                    even_load(d).wait()
                cross_copy(d, j).wait_recv()
                value = own_weight * even[d - 1, :, chunk(SUMMED[j])].astype(jnp.float32)
                value = value + partner_weight * cross_in[d, j].astype(jnp.float32)
                part_out[d - 1, j] = value.astype(jnp.bfloat16)
                part_copy(d, j).start()

    def relay_pair():
        @pl.when(col == 0)
        def _():
            first_load.wait()

        for d in steps:

            @pl.when(inward(d))
            def _():
                settle(raw_b.at[d - 1], raw_s.at[1, d - 1], raw_r.at[1, d - 1]).wait_recv()

        @pl.when(pair_sent)
        def _():
            weights = [weight(partner, 2 * d + 1 - 2 * col) for d in steps]
            first_weight = weight(partner, 1)
            for n, c in enumerate(PLAIN):
                value = first_weight * first[:, chunk(c)].astype(jnp.float32)
                for d in steps:
                    value = value + weights[d - 1] * raw_b[d - 1, n].astype(jnp.float32)
                pair_out[n] = value.astype(jnp.bfloat16)
                pair_copy(n).start()

    def gather_past(c):
        if c in SUMMED:
            j = SUMMED.index(c)

            @pl.when(col == 1)
            def _():
                cross_copy(0, j).wait_recv()

            for d in steps:

                @pl.when(inward(d))
                def _():
                    part_copy(d, j).wait_recv()

            value = weight(section, 1) * cross_in[0, j].astype(jnp.float32)
            for d in steps:
                value = value + part_in[d - 1, j].astype(jnp.float32)
        else:
            n = PLAIN.index(c)

            @pl.when(pair_due)
            def _():
                pair_copy(n).wait_recv()

            if n == 0:
                for d in steps:

                    @pl.when(inward(d))
                    def _():
                        settle(raw_a.at[d - 1], raw_s.at[0, d - 1], raw_r.at[0, d - 1]).wait_recv()

            value = pair_in[n].astype(jnp.float32)
            for d in steps:
                value = value + weight(section, 2 * d) * raw_a[d - 1, n].astype(jnp.float32)
        past[c] = value

    scale = 1.0 / math.sqrt(HEAD_DIM)

    def project(spans):
        def places():
            done = 0
            for block, first_row, size in spans:
                where = pl.ds(pl.multiple_of(block * rows + first_row, size), size)
                yield where, slice(done, done + size)
                done += size

        def tokens():
            taken = [rows_all[block, at : at + size, :] for block, at, size in spans]
            return taken[0] if len(taken) == 1 else jnp.concatenate(taken, axis=0)

        def q_tile(j, carry):
            acc = jnp.dot(tokens(), w_all[j], preferred_element_type=jnp.float32)
            acc = acc.astype(jnp.bfloat16) * jnp.bfloat16(scale)
            for where, got in places():
                q_all[2 * j, where, :] = acc[got, :half]
                q_all[2 * j + 1, where, :] = acc[got, half:]
            return carry

        lax.fori_loop(0, q_tiles, q_tile, 0)
        acc = jnp.dot(tokens(), w_all[q_tiles], preferred_element_type=jnp.float32)
        acc = acc.astype(jnp.bfloat16).astype(jnp.float32)
        for values, padded in ((acc[:, :half], k_pad), (acc[:, half:], v_pad)):
            lane = lax.broadcasted_iota(jnp.int32, values.shape, 1)
            turned = pltpu.roll(values, HEAD_DIM, 1)
            low = lane < HEAD_DIM
            zero = jnp.zeros_like(values)
            forms = (
                jnp.where(low, values, zero),
                jnp.where(low, zero, turned),
                jnp.where(low, turned, zero),
                jnp.where(low, zero, values),
            )
            for f, form in enumerate(forms):
                for where, got in places():
                    padded[f, where, pl.ds(0, half)] = form[got].astype(jnp.bfloat16)

    pairs = q_all.shape[0]
    pairs_per_kv = pairs // (half // HEAD_DIM)

    def attend(block, wanted, first_row, size):
        for b in range(4):
            keys = (b + 1) * rows
            at = b * rows + first_row

            @pl.when(wanted & (block == b))
            def _():
                with jax.named_scope(f"att{b}_{size}"):
                    shape = (pairs_per_kv, size, rows)
                    seen = (
                        lax.broadcasted_iota(jnp.int32, shape, 1) + first_row
                        >= lax.broadcasted_iota(jnp.int32, shape, 2)
                    ).reshape(pairs_per_kv * size, rows)
                    for kv in range(pairs // pairs_per_kv):
                        group = slice(kv * pairs_per_kv, (kv + 1) * pairs_per_kv)
                        query = q_all[group, at : at + size, :]
                        query = query.reshape(pairs_per_kv * size, half)
                        total = None
                        for which in range(2):
                            scores = lax.dot_general(
                                query,
                                k_pad[kv * 2 + which, :keys, :],
                                (((1,), (1,)), ((), ())),
                                preferred_element_type=jnp.float32,
                            )
                            last = jnp.where(seen, scores[:, b * rows :], -1e30)
                            if b:
                                scores = jnp.concatenate([scores[:, : b * rows], last], axis=1)
                            else:
                                scores = last
                            top = jnp.max(scores, axis=-1, keepdims=True)
                            weights = jnp.exp(scores - top).astype(jnp.bfloat16)
                            term = jnp.dot(
                                weights,
                                v_pad[kv * 2 + which, :keys, :],
                                preferred_element_type=jnp.float32,
                            )
                            term = term[:, :half] * (1.0 / term[:, half:])
                            total = term if total is None else total + term
                        total = total.astype(jnp.bfloat16)
                        for i in range(pairs_per_kv):
                            p = kv * pairs_per_kv + i
                            heads[b, first_row : first_row + size, p * half : (p + 1) * half] = (
                                total[i * size : (i + 1) * size]
                            )

    def part(block, c, first_row=0, size=rows):
        taken = heads[block, first_row : first_row + size, :]
        acc = jnp.dot(taken, w_out[c], preferred_element_type=jnp.float32)
        return acc.astype(jnp.bfloat16)

    short = rows // 2

    def far_copy(c, h, way):
        at = pl.ds(h * short, short)
        return pltpu.make_async_remote_copy(
            src_ref=far_send.at[c, at],
            dst_ref=relay_in.at[c, at],
            send_sem=far_s,
            recv_sem=far_r.at[c],
            device_id={"tensor": to[way]},
            device_id_type=MESH,
        )

    def near_copy(way, c):
        return pltpu.make_async_remote_copy(
            src_ref=near_send.at[way, c],
            dst_ref=final_in.at[way, c],
            send_sem=near_s,
            recv_sem=near_r.at[way, c],
            device_id={"tensor": to[way]},
            device_id_type=MESH,
        )

    def out_copy(c):
        return pltpu.make_async_remote_copy(
            src_ref=mixed.at[c],
            dst_ref=out_hbm.at[0, :, pl.ds(pl.multiple_of(c * cols, cols), cols)],
            send_sem=out_s,
            recv_sem=out_r,
            device_id={"section": nxt},
            device_id_type=MESH,
        )

    for copy in loads:
        copy.wait()
    project(((me, 0, rows),))

    def arrived(way, p):
        place = rows_all.at[source[way], pl.ds(p * piece, piece)]
        return pltpu.make_async_remote_copy(
            src_ref=place,
            dst_ref=place,
            send_sem=ag_s.at[way],
            recv_sem=ag_r.at[way, p],
            device_id={"tensor": to[way]},
            device_id_type=MESH,
        )

    for p in range(PIECES):
        for way in range(2):
            arrived(way, p).wait_recv()
            pass_copy(way, p).start()
        if p == 1:
            load_mix.wait()
            with jax.named_scope("relay0"):
                relay(0)
    with jax.named_scope("relay1"):
        relay(1)
    for copy in out_loads:
        copy.wait()
    with jax.named_scope("f_proj_near"):
        project(((left, 0, rows), (right, 0, rows)))
    attend(me, far > me, 0, rows)

    for h in range(2):
        for p in (2 * h, 2 * h + 1):
            for way in range(2):
                passed(way, p, far).wait_recv()
        with jax.named_scope(f"i_proj_far{h}"):
            project(((far, h * short, short),))
        with jax.named_scope(f"j_att_far{h}"):
            attend(far, True, h * short, short)

        def far_step(i, carry):
            at = pl.ds(h * short, short)
            far_send[i, at] = part(far, i, h * short, short)
            far_copy(i, h, 1).start()
            far_send[side + i, at] = part(far, side + i, h * short, short)
            far_copy(side + i, h, 0).start()
            return carry

        with jax.named_scope(f"k_far_step{h}"):
            lax.fori_loop(0, side, far_step, 0)
        if h == 0:
            with jax.named_scope("relay2"):
                relay(2)
            with jax.named_scope("relay_pair"):
                relay_pair()

    attend(right, True, 0, rows)
    attend(left, True, 0, rows)
    with jax.named_scope("relay3"):
        relay(3)

    def near_step(i, carry):
        def relayed(way):
            c = side + i if way == 0 else i
            value = part(to[way], c)
            settle(relay_in.at[c], far_s, far_r.at[c]).wait_recv()
            total = value.astype(jnp.float32) + relay_in[c].astype(jnp.float32)
            near_send[way, c] = total.astype(jnp.bfloat16)
            near_copy(way, c).start()

        def direct(way):
            c = i if way == 0 else side + i
            near_send[way, c] = part(to[way], c)
            near_copy(way, c).start()

        relayed(0)
        direct(1)
        relayed(1)
        direct(0)
        return carry

    lax.fori_loop(0, side, near_step, 0)
    attend(me, far < me, 0, rows)

    def own_step(c, carry):
        own_part[c] = part(me, c)
        return carry

    lax.fori_loop(0, col_chunks, own_step, 0)

    own_weight = weight(section, 0)

    for i in range(col_chunks):
        c = (i + 1) % 2 * side + i // 2
        with jax.named_scope(f"past{i}"):
            gather_past(c)
        with jax.named_scope(f"final{i}"):
            total = own_part[c].astype(jnp.float32)
            for way in range(2):
                near_copy(way, c).wait_recv()
                total = total + final_in[way, c].astype(jnp.float32)
            block = (x_own[:, chunk(c)].astype(jnp.float32) + total).astype(jnp.bfloat16)
            mixed[c] = (own_weight * block.astype(jnp.float32) + past[c]).astype(jnp.bfloat16)
            out_copy(c).start()
        if i == 1:
            with jax.named_scope("relay4"):
                relay(4)

    for way in range(2):
        settle(rows_all.at[me], ag_s.at[way], ag_r.at[way, 0]).wait_send()
        half_block = rows_all.at[me, :, pl.ds(0, width // 2)]
        settle(half_block, fw_s.at[way], fw_r.at[way, 0]).wait_send()

    for d in (0, *steps):

        @pl.when(cross_sent(d))
        def _():
            settle(cross_in.at[d], cross_s.at[d], cross_r.at[d, 0]).wait_send()

    for d in steps:

        @pl.when(onward(d))
        def _():
            settle(part_out.at[d - 1], part_s.at[d - 1], part_r.at[d - 1, 0]).wait_send()
            for which, raw in ((0, raw_a), (1, raw_b)):
                settle(raw.at[d - 1], raw_s.at[which, d - 1], raw_r.at[which, d - 1]).wait_send()

    @pl.when(pair_sent)
    def _():
        settle(pair_out, pair_s, pair_r.at[0]).wait_send()

    settle(far_send, far_s, far_r.at[0]).wait_send()
    settle(near_send, near_s, near_r.at[0, 0]).wait_send()
    with jax.named_scope("s_drain"):
        settle(mixed, out_s, out_r).wait_send()
        settle(out_hbm.at[0], out_s, out_r).wait_recv()


def solution(mesh):
    sections, tensor = mesh.shape["section"], mesh.shape["tensor"]
    assert tensor == 4 and sections == 32
    col_chunks = 8

    def on_device(x, history, wq, wk, wv, wo, mix_weights):
        rows, width = x.shape[1:]
        q_width, kv_width = wq.shape[2], wk.shape[2]
        seq = rows * tensor
        tile = 2 * kv_width
        q_tiles = q_width // tile
        cols = width // col_chunks
        summed, plain = len(SUMMED), len(PLAIN)
        bf16 = jnp.bfloat16
        dma = pltpu.SemaphoreType.DMA
        hbm = pl.BlockSpec(memory_space=pl.ANY)
        return pl.pallas_call(
            functools.partial(tick_kernel, sections),
            out_shape=jax.ShapeDtypeStruct(x.shape, bf16),
            in_specs=[hbm] * 7,
            out_specs=hbm,
            scratch_shapes=[
                pltpu.VMEM((rows, width), bf16),
                pltpu.VMEM((tensor, rows, width), bf16),
                pltpu.VMEM((q_tiles + 1, width, tile), bf16),
                pltpu.VMEM((col_chunks, q_width, cols), bf16),
                pltpu.VMEM((2 * q_tiles, seq, kv_width), bf16),
                pltpu.VMEM((4, seq, kv_width), bf16),
                pltpu.VMEM((4, seq, 2 * kv_width), bf16),
                pltpu.VMEM((tensor, rows, q_width), bf16),
                pltpu.VMEM((col_chunks, rows, cols), bf16),
                pltpu.VMEM((col_chunks, rows, cols), bf16),
                pltpu.VMEM((2, col_chunks, rows, cols), bf16),
                pltpu.VMEM((2, col_chunks, rows, cols), bf16),
                pltpu.VMEM((col_chunks, rows, cols), bf16),
                pltpu.VMEM((col_chunks, rows, cols), bf16),
                pltpu.VMEM((3, rows, width), bf16),
                pltpu.VMEM((4, summed, rows, cols), bf16),
                pltpu.VMEM((3, summed, rows, cols), bf16),
                pltpu.VMEM((3, summed, rows, cols), bf16),
                pltpu.VMEM((3, plain, rows, cols), bf16),
                pltpu.VMEM((3, plain, rows, cols), bf16),
                pltpu.VMEM((rows, width), bf16),
                pltpu.VMEM((plain, rows, cols), bf16),
                pltpu.VMEM((plain, rows, cols), bf16),
                pltpu.VMEM((col_chunks, rows, cols), jnp.float32),
                pltpu.VMEM(mix_weights.shape[::-1], mix_weights.dtype),
                dma((q_tiles + 2,)),
                dma((col_chunks,)),
                dma((PIECES,)),
                dma,
                dma((3,)),
                dma,
                dma((4,)),
                dma((4, summed)),
                dma((3,)),
                dma((3, summed)),
                dma((2, 3)),
                dma((2, 3)),
                dma,
                dma((plain,)),
                dma((2,)),
                dma((2, PIECES)),
                dma((2,)),
                dma((2, PIECES)),
                dma,
                dma((col_chunks,)),
                dma,
                dma((2, col_chunks)),
                dma,
                dma,
            ],
            compiler_params=pltpu.CompilerParams(
                collective_id=0, has_side_effects=True, vmem_limit_bytes=60 * 1024 * 1024
            ),
        )(x, history, wq, wk, wv, wo, mix_weights.T)

    placed = (
        P("section", "tensor", None),
        P("section", None, "tensor", None),
        P("section", None, "tensor"),
        P("section", None, "tensor"),
        P("section", None, "tensor"),
        P("section", "tensor", None),
        P(),
    )
    return jax.shard_map(
        on_device,
        mesh=mesh,
        in_specs=placed,
        out_specs=P("section", "tensor", None),
        check_vma=False,
    )
```

```python
import functools
import math

import jax
import jax.numpy as jnp
from jax import lax
from jax.experimental import pallas as pl
from jax.experimental.pallas import tpu as pltpu
from jax.sharding import PartitionSpec as P

HEAD_DIM = 64
SUMMED = (4, 0, 5, 1, 3)
PLAIN = (6, 2, 7)
MESH = pl.DeviceIdType.MESH
PIECES = 4


def start(copy):
    copy.start()
    return copy


def tick_kernel(
    sections,
    x_hbm,
    hist_hbm,
    wq_hbm,
    wk_hbm,
    wv_hbm,
    wo_hbm,
    mix_hbm,
    out_hbm,
    x_own,
    rows_all,
    w_all,
    w_out,
    q_all,
    k_pad,
    v_pad,
    heads,
    far_send,
    relay_in,
    near_send,
    final_in,
    own_part,
    mixed,
    even,
    cross_in,
    part_out,
    part_in,
    raw_a,
    raw_b,
    first,
    pair_out,
    pair_in,
    past,
    mix_v,
    w_sem,
    wo_sem,
    x_sem,
    mix_sem,
    even_sem,
    first_sem,
    cross_s,
    cross_r,
    part_s,
    part_r,
    raw_s,
    raw_r,
    pair_s,
    pair_r,
    ag_s,
    ag_r,
    fw_s,
    fw_r,
    far_s,
    far_r,
    near_s,
    near_r,
    out_s,
    out_r,
):
    section = lax.axis_index("section")
    me = lax.axis_index("tensor")
    right, left, far = lax.rem(me + 1, 4), lax.rem(me + 3, 4), lax.rem(me + 2, 4)
    to = (right, left)
    source = (left, right)
    rows, width = x_own.shape
    piece = rows // PIECES
    q_tiles = w_all.shape[0] - 1
    tile = w_all.shape[2]
    half = tile // 2
    col_chunks, _, cols = w_out.shape
    side = col_chunks // 2
    nxt = lax.rem(section + 1, sections)
    prv = lax.rem(section + sections - 1, sections)

    def load_x(p):
        at = pl.ds(p * piece, piece)
        return pltpu.make_async_copy(x_hbm.at[0, at], x_own.at[at], x_sem.at[p])

    for p in range(PIECES):
        load_x(p).start()
    barrier = pltpu.get_barrier_semaphore()
    for other in to:
        pl.semaphore_signal(barrier, inc=1, device_id={"tensor": other}, device_id_type=MESH)
    row, col = section // 8, lax.rem(section // 4, 2)
    partner = section + 4 - 8 * col
    others = [lax.rem(section + 8 * d, sections) for d in (1, 2, 3)]
    for other in (nxt, prv, partner, *others):
        pl.semaphore_signal(barrier, inc=1, device_id={"section": other}, device_id_type=MESH)

    loads = []
    for j in range(q_tiles):
        loads.append(
            pltpu.make_async_copy(
                wq_hbm.at[0, :, pl.ds(j * tile, tile)], w_all.at[j], w_sem.at[j]
            )
        )
    loads.append(
        pltpu.make_async_copy(
            wk_hbm.at[0], w_all.at[q_tiles, :, pl.ds(0, half)], w_sem.at[q_tiles]
        )
    )
    loads.append(
        pltpu.make_async_copy(
            wv_hbm.at[0], w_all.at[q_tiles, :, pl.ds(half, half)], w_sem.at[q_tiles + 1]
        )
    )
    load_x(0).wait()
    for copy in loads:
        copy.start()
    load_mix = start(pltpu.make_async_copy(mix_hbm, mix_v, mix_sem))

    def own_copy(way, p):
        place = rows_all.at[me, pl.ds(p * piece, piece)]
        return pltpu.make_async_remote_copy(
            src_ref=place,
            dst_ref=place,
            send_sem=ag_s.at[way],
            recv_sem=ag_r.at[way, p],
            device_id={"tensor": to[way]},
            device_id_type=MESH,
        )

    def settle(ref, send, recv):
        return pltpu.make_async_remote_copy(
            src_ref=ref,
            dst_ref=ref,
            send_sem=send,
            recv_sem=recv,
            device_id={"tensor": right},
            device_id_type=MESH,
        )

    def passed(way, p, block):
        place = rows_all.at[
            block, pl.ds(p * piece, piece), pl.ds(way * (width // 2), width // 2)
        ]
        return pltpu.make_async_remote_copy(
            src_ref=place,
            dst_ref=place,
            send_sem=fw_s.at[way],
            recv_sem=fw_r.at[p // 2],
            device_id={"tensor": to[way]},
            device_id_type=MESH,
        )

    def pass_copy(way, p):
        return passed(way, p, source[way])

    def norm_piece(p):
        def norm_rows(i, carry):
            at = pl.ds(pl.multiple_of(p * piece + i * 16, 16), 16)
            values = x_own[at, :].astype(jnp.float32)
            inv = lax.rsqrt(jnp.mean(values * values, axis=-1, keepdims=True) + 1e-05)
            rows_all[me, at, :] = (values * inv).astype(jnp.bfloat16)
            return carry

        lax.fori_loop(0, piece // 16, norm_rows, 0)

    norm_piece(0)
    pl.semaphore_wait(barrier, 8)
    for p in range(PIECES):
        if p:
            load_x(p).wait()
            norm_piece(p)
        own_copy(0, p).start()
        own_copy(1, p).start()

    steps = range(1, 4)

    def chunk(c):
        return pl.ds(c * cols, cols)

    def onward(d):
        return row + d < 4

    def inward(d):
        return row >= d

    def cross_sent(d):
        return onward(d) if d else col == 0

    def cross_due(d):
        return onward(d) if d else col == 1

    def section_copy(src, dst, send, recv, target):
        return pltpu.make_async_remote_copy(
            src_ref=src,
            dst_ref=dst,
            send_sem=send,
            recv_sem=recv,
            device_id={"section": target},
            device_id_type=MESH,
        )

    def cross_copy(d, j):
        return section_copy(
            hist_hbm.at[0, jnp.maximum(2 * d - 2 * col, 0), :, chunk(SUMMED[j])],
            cross_in.at[d, j],
            cross_s.at[d],
            cross_r.at[0 if d else 1, j],
            partner,
        )

    def part_copy(d, j):
        return section_copy(
            part_out.at[d - 1, j],
            part_in.at[d - 1, j],
            part_s.at[d - 1],
            part_r.at[j],
            others[d - 1],
        )

    def raw_copy(d, which, n):
        slot = 2 * d - 1 if which == 0 else 2 * d - 2 * col
        return section_copy(
            hist_hbm.at[0, slot, :, chunk(PLAIN[n])],
            (raw_a, raw_b)[which].at[d - 1, n],
            raw_s.at[which, d - 1],
            raw_r.at[which, d - 1],
            others[d - 1],
        )

    def pair_copy(n):
        return section_copy(pair_out.at[n], pair_in.at[n], pair_s, pair_r.at[n], partner)

    pair_sent = (row >= 1) | (col == 0)
    pair_due = (row >= 1) | (col == 1)

    def even_load(d):
        return pltpu.make_async_copy(
            hist_hbm.at[0, 2 * d - 1], even.at[d - 1], even_sem.at[d - 1]
        )

    first_load = pltpu.make_async_copy(hist_hbm.at[0, 0], first, first_sem)

    def cross(some):
        for j in some:
            for d in (1, 2, 3, 0):

                @pl.when(cross_sent(d))
                def _():
                    cross_copy(d, j).start()

    cross(range(len(SUMMED)))

    for which in (1, 0):
        for d in steps:

            @pl.when(onward(d))
            def _():
                for n in range(len(PLAIN)):
                    raw_copy(d, which, n).start()

    out_loads = []
    for c in range(col_chunks):
        out_loads.append(
            start(
                pltpu.make_async_copy(
                    wo_hbm.at[0, :, pl.ds(c * cols, cols)], w_out.at[c], wo_sem.at[c]
                )
            )
        )

    for d in steps:

        @pl.when(onward(d))
        def _():
            even_load(d).start()

        @pl.when(row < d)
        def _():
            part_in[d - 1] = jnp.zeros(part_in.shape[1:], part_in.dtype)
            raw_a[d - 1] = jnp.zeros(raw_a.shape[1:], raw_a.dtype)
            raw_b[d - 1] = jnp.zeros(raw_b.shape[1:], raw_b.dtype)

    @pl.when(col == 0)
    def _():
        first_load.start()
        cross_in[0] = jnp.zeros(cross_in.shape[1:], cross_in.dtype)

    @pl.when(col == 1)
    def _():
        first[...] = jnp.zeros(first.shape, first.dtype)

    @pl.when(jnp.logical_not(pair_due))
    def _():
        pair_in[...] = jnp.zeros(pair_in.shape, pair_in.dtype)

    k_pad[...] = jnp.zeros(k_pad.shape, k_pad.dtype)
    for f in range(v_pad.shape[0]):
        v_pad[f, :, :half] = jnp.zeros((v_pad.shape[1], half), v_pad.dtype)
        v_pad[f, :, half:] = jnp.ones((v_pad.shape[1], half), v_pad.dtype)

    def weight(target, k):
        table = mix_v[...]
        at = (lax.broadcasted_iota(jnp.int32, table.shape, 0) == k) & (
            lax.broadcasted_iota(jnp.int32, table.shape, 1) == target
        )
        return jnp.sum(jnp.where(at, table, 0.0), keepdims=True)

    def relay(j):
        for count in steps:

            @pl.when(row == 3 - count)
            def _():
                settle(cross_in.at[pl.ds(1, count), j], cross_s.at[1], cross_r.at[0, j]).wait_recv()

        for d in steps:

            @pl.when(onward(d))
            def _():
                own_weight = weight(section + 8 * d, 2 * d)
                partner_weight = weight(section + 8 * d, 2 * d - 1 + 2 * col)
                if j == 0:
                    even_load(d).wait()
                value = own_weight * even[d - 1, :, chunk(SUMMED[j])].astype(jnp.float32)
                value = value + partner_weight * cross_in[d, j].astype(jnp.float32)
                part_out[d - 1, j] = value.astype(jnp.bfloat16)
                part_copy(d, j).start()

    def relay_pair():
        @pl.when(col == 0)
        def _():
            first_load.wait()

        for d in steps:

            @pl.when(inward(d))
            def _():
                settle(raw_b.at[d - 1], raw_s.at[1, d - 1], raw_r.at[1, d - 1]).wait_recv()

        @pl.when(pair_sent)
        def _():
            weights = [weight(partner, 2 * d + 1 - 2 * col) for d in steps]
            first_weight = weight(partner, 1)
            for n, c in enumerate(PLAIN):
                value = first_weight * first[:, chunk(c)].astype(jnp.float32)
                for d in steps:
                    value = value + weights[d - 1] * raw_b[d - 1, n].astype(jnp.float32)
                pair_out[n] = value.astype(jnp.bfloat16)
                pair_copy(n).start()

    def gather_past(c):
        if c in SUMMED:
            j = SUMMED.index(c)

            @pl.when(col == 1)
            def _():
                cross_copy(0, j).wait_recv()

            for count in steps:

                @pl.when(row == count)
                def _():
                    settle(part_in.at[pl.ds(0, count), j], part_s.at[0], part_r.at[j]).wait_recv()

            value = weight(section, 1) * cross_in[0, j].astype(jnp.float32)
            for d in steps:
                value = value + part_in[d - 1, j].astype(jnp.float32)
        else:
            n = PLAIN.index(c)

            @pl.when(pair_due)
            def _():
                pair_copy(n).wait_recv()

            if n == 0:
                for d in steps:

                    @pl.when(inward(d))
                    def _():
                        settle(raw_a.at[d - 1], raw_s.at[0, d - 1], raw_r.at[0, d - 1]).wait_recv()

            value = pair_in[n].astype(jnp.float32)
            for d in steps:
                value = value + weight(section, 2 * d) * raw_a[d - 1, n].astype(jnp.float32)
        past[c] = value

    scale = 1.0 / math.sqrt(HEAD_DIM)

    def project(spans):
        def places():
            done = 0
            for block, first_row, size in spans:
                where = pl.ds(pl.multiple_of(block * rows + first_row, size), size)
                yield where, slice(done, done + size)
                done += size

        def tokens():
            taken = [rows_all[block, at : at + size, :] for block, at, size in spans]
            return taken[0] if len(taken) == 1 else jnp.concatenate(taken, axis=0)

        def q_tile(j, carry):
            acc = jnp.dot(tokens(), w_all[j], preferred_element_type=jnp.float32)
            acc = acc.astype(jnp.bfloat16) * jnp.bfloat16(scale)
            for where, got in places():
                q_all[2 * j, where, :] = acc[got, :half]
                q_all[2 * j + 1, where, :] = acc[got, half:]
            return carry

        lax.fori_loop(0, q_tiles, q_tile, 0)
        acc = jnp.dot(tokens(), w_all[q_tiles], preferred_element_type=jnp.float32)
        acc = acc.astype(jnp.bfloat16).astype(jnp.float32)
        for values, padded in ((acc[:, :half], k_pad), (acc[:, half:], v_pad)):
            lane = lax.broadcasted_iota(jnp.int32, values.shape, 1)
            turned = pltpu.roll(values, HEAD_DIM, 1)
            low = lane < HEAD_DIM
            zero = jnp.zeros_like(values)
            forms = (
                jnp.where(low, values, zero),
                jnp.where(low, zero, turned),
                jnp.where(low, turned, zero),
                jnp.where(low, zero, values),
            )
            for f, form in enumerate(forms):
                for where, got in places():
                    padded[f, where, pl.ds(0, half)] = form[got].astype(jnp.bfloat16)

    pairs = q_all.shape[0]
    pairs_per_kv = pairs // (half // HEAD_DIM)

    def attend(block, wanted, first_row, size):
        for b in range(4):
            keys = (b + 1) * rows
            at = b * rows + first_row

            @pl.when(wanted & (block == b))
            def _():
                with jax.named_scope(f"att{b}_{size}"):
                    shape = (pairs_per_kv, size, rows)
                    seen = (
                        lax.broadcasted_iota(jnp.int32, shape, 1) + first_row
                        >= lax.broadcasted_iota(jnp.int32, shape, 2)
                    ).reshape(pairs_per_kv * size, rows)
                    for kv in range(pairs // pairs_per_kv):
                        group = slice(kv * pairs_per_kv, (kv + 1) * pairs_per_kv)
                        query = q_all[group, at : at + size, :]
                        query = query.reshape(pairs_per_kv * size, half)
                        total = None
                        for which in range(2):
                            scores = lax.dot_general(
                                query,
                                k_pad[kv * 2 + which, :keys, :],
                                (((1,), (1,)), ((), ())),
                                preferred_element_type=jnp.float32,
                            )
                            last = jnp.where(seen, scores[:, b * rows :], -1e30)
                            if b:
                                scores = jnp.concatenate([scores[:, : b * rows], last], axis=1)
                            else:
                                scores = last
                            top = jnp.max(scores, axis=-1, keepdims=True)
                            weights = jnp.exp(scores - top).astype(jnp.bfloat16)
                            term = jnp.dot(
                                weights,
                                v_pad[kv * 2 + which, :keys, :],
                                preferred_element_type=jnp.float32,
                            )
                            term = term[:, :half] * (1.0 / term[:, half:])
                            total = term if total is None else total + term
                        total = total.astype(jnp.bfloat16)
                        for i in range(pairs_per_kv):
                            p = kv * pairs_per_kv + i
                            heads[b, first_row : first_row + size, p * half : (p + 1) * half] = (
                                total[i * size : (i + 1) * size]
                            )

    def part(block, c, first_row=0, size=rows):
        taken = heads[block, first_row : first_row + size, :]
        acc = jnp.dot(taken, w_out[c], preferred_element_type=jnp.float32)
        return acc.astype(jnp.bfloat16)

    short = rows // 2

    def far_copy(c, h, way):
        at = pl.ds(h * short, short)
        return pltpu.make_async_remote_copy(
            src_ref=far_send.at[c, at],
            dst_ref=relay_in.at[c, at],
            send_sem=far_s,
            recv_sem=far_r.at[c],
            device_id={"tensor": to[way]},
            device_id_type=MESH,
        )

    def near_copy(way, c):
        return pltpu.make_async_remote_copy(
            src_ref=near_send.at[way, c],
            dst_ref=final_in.at[way, c],
            send_sem=near_s,
            recv_sem=near_r.at[c],
            device_id={"tensor": to[way]},
            device_id_type=MESH,
        )

    def out_copy(c):
        return pltpu.make_async_remote_copy(
            src_ref=mixed.at[c],
            dst_ref=out_hbm.at[0, :, pl.ds(pl.multiple_of(c * cols, cols), cols)],
            send_sem=out_s,
            recv_sem=out_r,
            device_id={"section": nxt},
            device_id_type=MESH,
        )

    for copy in loads:
        copy.wait()
    project(((me, 0, rows),))

    def arrived(way, p):
        place = rows_all.at[source[way], pl.ds(p * piece, piece)]
        return pltpu.make_async_remote_copy(
            src_ref=place,
            dst_ref=place,
            send_sem=ag_s.at[way],
            recv_sem=ag_r.at[way, p],
            device_id={"tensor": to[way]},
            device_id_type=MESH,
        )

    for p in range(PIECES):
        for way in range(2):
            arrived(way, p).wait_recv()
            pass_copy(way, p).start()
        if p == 1:
            load_mix.wait()
            with jax.named_scope("relay0"):
                relay(0)
    with jax.named_scope("relay1"):
        relay(1)
    for copy in out_loads:
        copy.wait()
    with jax.named_scope("f_proj_near"):
        project(((left, 0, rows), (right, 0, rows)))
    attend(me, far > me, 0, rows)

    for h in range(2):
        settle(rows_all.at[far, pl.ds(h * short, short)], fw_s.at[0], fw_r.at[h]).wait_recv()
        with jax.named_scope(f"i_proj_far{h}"):
            project(((far, h * short, short),))
        with jax.named_scope(f"j_att_far{h}"):
            attend(far, True, h * short, short)

        def far_step(i, carry):
            at = pl.ds(h * short, short)
            far_send[i, at] = part(far, i, h * short, short)
            far_copy(i, h, 1).start()
            far_send[side + i, at] = part(far, side + i, h * short, short)
            far_copy(side + i, h, 0).start()
            return carry

        with jax.named_scope(f"k_far_step{h}"):
            lax.fori_loop(0, side, far_step, 0)
        if h == 0:
            with jax.named_scope("relay2"):
                relay(2)
            with jax.named_scope("relay_pair"):
                relay_pair()

    attend(right, True, 0, rows)
    attend(left, True, 0, rows)
    with jax.named_scope("relay3"):
        relay(3)

    def near_step(i, carry):
        def relayed(way):
            c = side + i if way == 0 else i
            value = part(to[way], c)
            settle(relay_in.at[c], far_s, far_r.at[c]).wait_recv()
            total = value.astype(jnp.float32) + relay_in[c].astype(jnp.float32)
            near_send[way, c] = total.astype(jnp.bfloat16)
            near_copy(way, c).start()

        def direct(way):
            c = i if way == 0 else side + i
            near_send[way, c] = part(to[way], c)
            near_copy(way, c).start()

        relayed(0)
        direct(1)
        relayed(1)
        direct(0)
        return carry

    lax.fori_loop(0, side, near_step, 0)
    attend(me, far < me, 0, rows)

    def own_step(c, carry):
        own_part[c] = part(me, c)
        return carry

    lax.fori_loop(0, col_chunks, own_step, 0)

    own_weight = weight(section, 0)

    for i in range(col_chunks):
        c = (i + 1) % 2 * side + i // 2
        with jax.named_scope(f"past{i}"):
            gather_past(c)
        with jax.named_scope(f"final{i}"):
            total = own_part[c].astype(jnp.float32)
            settle(final_in.at[:, c], near_s, near_r.at[c]).wait_recv()
            for way in range(2):
                total = total + final_in[way, c].astype(jnp.float32)
            block = (x_own[:, chunk(c)].astype(jnp.float32) + total).astype(jnp.bfloat16)
            mixed[c] = (own_weight * block.astype(jnp.float32) + past[c]).astype(jnp.bfloat16)
            out_copy(c).start()
        if i == 1:
            with jax.named_scope("relay4"):
                relay(4)

    for way in range(2):
        settle(rows_all.at[me], ag_s.at[way], ag_r.at[way, 0]).wait_send()
        half_block = rows_all.at[me, :, pl.ds(0, width // 2)]
        settle(half_block, fw_s.at[way], fw_r.at[0]).wait_send()

    for d in (0, *steps):

        @pl.when(cross_sent(d))
        def _():
            settle(cross_in.at[d], cross_s.at[d], cross_r.at[0, 0]).wait_send()

    for d in steps:

        @pl.when(onward(d))
        def _():
            settle(part_out.at[d - 1], part_s.at[d - 1], part_r.at[0]).wait_send()
            for which, raw in ((0, raw_a), (1, raw_b)):
                settle(raw.at[d - 1], raw_s.at[which, d - 1], raw_r.at[which, d - 1]).wait_send()

    @pl.when(pair_sent)
    def _():
        settle(pair_out, pair_s, pair_r.at[0]).wait_send()

    settle(far_send, far_s, far_r.at[0]).wait_send()
    settle(near_send, near_s, near_r.at[0]).wait_send()
    with jax.named_scope("s_drain"):
        settle(mixed, out_s, out_r).wait_send()
        settle(out_hbm.at[0], out_s, out_r).wait_recv()


def solution(mesh):
    sections, tensor = mesh.shape["section"], mesh.shape["tensor"]
    assert tensor == 4 and sections == 32
    col_chunks = 8

    def on_device(x, history, wq, wk, wv, wo, mix_weights):
        rows, width = x.shape[1:]
        q_width, kv_width = wq.shape[2], wk.shape[2]
        seq = rows * tensor
        tile = 2 * kv_width
        q_tiles = q_width // tile
        cols = width // col_chunks
        summed, plain = len(SUMMED), len(PLAIN)
        bf16 = jnp.bfloat16
        dma = pltpu.SemaphoreType.DMA
        hbm = pl.BlockSpec(memory_space=pl.ANY)
        return pl.pallas_call(
            functools.partial(tick_kernel, sections),
            out_shape=pltpu.VMEM(x.shape, bf16),
            in_specs=[hbm] * 7,
            out_specs=hbm,
            scratch_shapes=[
                pltpu.VMEM((rows, width), bf16),
                pltpu.VMEM((tensor, rows, width), bf16),
                pltpu.VMEM((q_tiles + 1, width, tile), bf16),
                pltpu.VMEM((col_chunks, q_width, cols), bf16),
                pltpu.VMEM((2 * q_tiles, seq, kv_width), bf16),
                pltpu.VMEM((4, seq, kv_width), bf16),
                pltpu.VMEM((4, seq, 2 * kv_width), bf16),
                pltpu.VMEM((tensor, rows, q_width), bf16),
                pltpu.VMEM((col_chunks, rows, cols), bf16),
                pltpu.VMEM((col_chunks, rows, cols), bf16),
                pltpu.VMEM((2, col_chunks, rows, cols), bf16),
                pltpu.VMEM((2, col_chunks, rows, cols), bf16),
                pltpu.VMEM((col_chunks, rows, cols), bf16),
                pltpu.VMEM((col_chunks, rows, cols), bf16),
                pltpu.VMEM((3, rows, width), bf16),
                pltpu.VMEM((4, summed, rows, cols), bf16),
                pltpu.VMEM((3, summed, rows, cols), bf16),
                pltpu.VMEM((3, summed, rows, cols), bf16),
                pltpu.VMEM((3, plain, rows, cols), bf16),
                pltpu.VMEM((3, plain, rows, cols), bf16),
                pltpu.VMEM((rows, width), bf16),
                pltpu.VMEM((plain, rows, cols), bf16),
                pltpu.VMEM((plain, rows, cols), bf16),
                pltpu.VMEM((col_chunks, rows, cols), jnp.float32),
                pltpu.VMEM(mix_weights.shape[::-1], mix_weights.dtype),
                dma((q_tiles + 2,)),
                dma((col_chunks,)),
                dma((PIECES,)),
                dma,
                dma((3,)),
                dma,
                dma((4,)),
                dma((2, summed)),
                dma((3,)),
                dma((summed,)),
                dma((2, 3)),
                dma((2, 3)),
                dma,
                dma((plain,)),
                dma((2,)),
                dma((2, PIECES)),
                dma((2,)),
                dma((2,)),
                dma,
                dma((col_chunks,)),
                dma,
                dma((col_chunks,)),
                dma,
                dma,
            ],
            compiler_params=pltpu.CompilerParams(
                collective_id=0, has_side_effects=True, vmem_limit_bytes=60 * 1024 * 1024
            ),
        )(x, history, wq, wk, wv, wo, mix_weights.T)

    placed = (
        P("section", "tensor", None),
        P("section", None, "tensor", None),
        P("section", None, "tensor"),
        P("section", None, "tensor"),
        P("section", None, "tensor"),
        P("section", "tensor", None),
        P(),
    )
    return jax.shard_map(
        on_device,
        mesh=mesh,
        in_specs=placed,
        out_specs=P("section", "tensor", None),
        check_vma=False,
    )
```

```python
import functools
import math

import jax
import jax.numpy as jnp
from jax import lax
from jax.experimental import pallas as pl
from jax.experimental.pallas import tpu as pltpu
from jax.sharding import PartitionSpec as P

HEAD_DIM = 64
ORDER = (4, 0, 5, 1, 6, 2, 7, 3)
SUMMED = {1: range(0, 3), 2: range(0, 8), 3: range(6, 8)}
PLAIN = {1: range(3, 8), 3: range(0, 6)}
MESH = pl.DeviceIdType.MESH
PIECES = 4


def start(copy):
    copy.start()
    return copy


def tick_kernel(
    sections,
    x_hbm,
    hist_hbm,
    wq_hbm,
    wk_hbm,
    wv_hbm,
    wo_hbm,
    mix_hbm,
    out_hbm,
    x_own,
    rows_all,
    w_all,
    w_out,
    q_all,
    k_pad,
    v_pad,
    heads,
    far_send,
    relay_in,
    near_send,
    final_in,
    own_part,
    mixed,
    even,
    cross_in,
    part_out,
    part_in,
    raw_a,
    raw_b,
    first,
    pair_out,
    pair_in,
    past,
    mix_v,
    w_sem,
    wo_sem,
    x_sem,
    mix_sem,
    even_sem,
    first_sem,
    cross_s,
    cross_r,
    part_s,
    part_r,
    raw_s,
    raw_r,
    pair_s,
    pair_r,
    ag_s,
    ag_r,
    fw_s,
    fw_r,
    far_s,
    far_r,
    near_s,
    near_r,
    out_s,
    out_r,
):
    section = lax.axis_index("section")
    me = lax.axis_index("tensor")
    right, left, far = lax.rem(me + 1, 4), lax.rem(me + 3, 4), lax.rem(me + 2, 4)
    to = (right, left)
    source = (left, right)
    rows, width = x_own.shape
    piece = rows // PIECES
    q_tiles = w_all.shape[0] - 1
    tile = w_all.shape[2]
    half = tile // 2
    col_chunks, _, cols = w_out.shape
    side = col_chunks // 2
    nxt = lax.rem(section + 1, sections)
    prv = lax.rem(section + sections - 1, sections)

    def load_x(p):
        at = pl.ds(p * piece, piece)
        return pltpu.make_async_copy(x_hbm.at[0, at], x_own.at[at], x_sem.at[p])

    for p in range(PIECES):
        load_x(p).start()
    barrier = pltpu.get_barrier_semaphore()
    for other in to:
        pl.semaphore_signal(barrier, inc=1, device_id={"tensor": other}, device_id_type=MESH)
    row, col = section // 8, lax.rem(section // 4, 2)
    partner = section + 4 - 8 * col
    others = [lax.rem(section + 8 * d, sections) for d in (1, 2, 3)]
    for other in (nxt, prv, partner, *others):
        pl.semaphore_signal(barrier, inc=1, device_id={"section": other}, device_id_type=MESH)

    loads = []
    for j in range(q_tiles):
        loads.append(
            pltpu.make_async_copy(
                wq_hbm.at[0, :, pl.ds(j * tile, tile)], w_all.at[j], w_sem.at[j]
            )
        )
    loads.append(
        pltpu.make_async_copy(
            wk_hbm.at[0], w_all.at[q_tiles, :, pl.ds(0, half)], w_sem.at[q_tiles]
        )
    )
    loads.append(
        pltpu.make_async_copy(
            wv_hbm.at[0], w_all.at[q_tiles, :, pl.ds(half, half)], w_sem.at[q_tiles + 1]
        )
    )
    load_x(0).wait()
    for copy in loads:
        copy.start()
    load_mix = start(pltpu.make_async_copy(mix_hbm, mix_v, mix_sem))

    def own_copy(way, p):
        place = rows_all.at[me, pl.ds(p * piece, piece)]
        return pltpu.make_async_remote_copy(
            src_ref=place,
            dst_ref=place,
            send_sem=ag_s.at[way],
            recv_sem=ag_r.at[way, p],
            device_id={"tensor": to[way]},
            device_id_type=MESH,
        )

    def settle(ref, send, recv):
        return pltpu.make_async_remote_copy(
            src_ref=ref,
            dst_ref=ref,
            send_sem=send,
            recv_sem=recv,
            device_id={"tensor": right},
            device_id_type=MESH,
        )

    def passed(way, p, block):
        place = rows_all.at[
            block, pl.ds(p * piece, piece), pl.ds(way * (width // 2), width // 2)
        ]
        return pltpu.make_async_remote_copy(
            src_ref=place,
            dst_ref=place,
            send_sem=fw_s.at[way],
            recv_sem=fw_r.at[p // 2],
            device_id={"tensor": to[way]},
            device_id_type=MESH,
        )

    def pass_copy(way, p):
        return passed(way, p, source[way])

    def norm_piece(p):
        def norm_rows(i, carry):
            at = pl.ds(pl.multiple_of(p * piece + i * 16, 16), 16)
            values = x_own[at, :].astype(jnp.float32)
            inv = lax.rsqrt(jnp.mean(values * values, axis=-1, keepdims=True) + 1e-05)
            rows_all[me, at, :] = (values * inv).astype(jnp.bfloat16)
            return carry

        lax.fori_loop(0, piece // 16, norm_rows, 0)

    norm_piece(0)
    pl.semaphore_wait(barrier, 8)
    for p in range(PIECES):
        if p:
            load_x(p).wait()
            norm_piece(p)
        own_copy(0, p).start()
        own_copy(1, p).start()

    steps = range(1, 4)

    def chunk(c):
        return pl.ds(c * cols, cols)

    def onward(d):
        return row + d < 4

    def inward(d):
        return row >= d

    def section_copy(src, dst, send, recv, target):
        return pltpu.make_async_remote_copy(
            src_ref=src,
            dst_ref=dst,
            send_sem=send,
            recv_sem=recv,
            device_id={"section": target},
            device_id_type=MESH,
        )

    def cross_copy(d, i):
        return section_copy(
            hist_hbm.at[0, jnp.maximum(2 * d - 2 * col, 0), :, chunk(ORDER[i])],
            cross_in.at[d - 1, i],
            cross_s.at[d - 1],
            cross_r.at[d - 1, i],
            partner,
        )

    def part_copy(d, i):
        return section_copy(
            part_out.at[d - 1, i],
            part_in.at[d - 1, i],
            part_s.at[d - 1],
            part_r.at[d - 1, i],
            others[d - 1],
        )

    def raw_copy(d, which, i):
        slot = 2 * d - 1 if which == 0 else 2 * d - 2 * col
        return section_copy(
            hist_hbm.at[0, slot, :, chunk(ORDER[i])],
            (raw_a, raw_b)[which].at[d - 1, i],
            raw_s.at[which, d - 1],
            raw_r.at[d - 1, i if which == 0 else col_chunks],
            others[d - 1],
        )

    def plain(d):
        return pl.ds(PLAIN[d].start, len(PLAIN[d]))

    def raw_wait(d, which):
        raw = (raw_a, raw_b)[which].at[d - 1, plain(d)]
        return settle(raw, raw_s.at[which, d - 1], raw_r.at[d - 1, col_chunks])

    def pair_copy(i):
        return section_copy(pair_out.at[i], pair_in.at[i], pair_s, pair_r.at[i], partner)

    pair_sent = (row >= 1) | (col == 0)
    pair_due = (row >= 1) | (col == 1)

    def even_load(d):
        return pltpu.make_async_copy(
            hist_hbm.at[0, 2 * d - 1], even.at[d - 1], even_sem.at[d - 1]
        )

    first_load = pltpu.make_async_copy(hist_hbm.at[0, 0], first, first_sem)

    for i in range(col_chunks):
        for d in steps:
            if i in SUMMED[d]:

                @pl.when(onward(d))
                def _():
                    cross_copy(d, i).start()

    for which in (1, 0):
        for d in (1, 3):

            @pl.when(onward(d))
            def _():
                for i in PLAIN[d]:
                    raw_copy(d, which, i).start()

    out_loads = []
    for c in range(col_chunks):
        out_loads.append(
            start(
                pltpu.make_async_copy(
                    wo_hbm.at[0, :, pl.ds(c * cols, cols)], w_out.at[c], wo_sem.at[c]
                )
            )
        )

    for d in steps:

        @pl.when(onward(d))
        def _():
            even_load(d).start()

        @pl.when(row < d)
        def _():
            for i in range(col_chunks):
                if i in SUMMED[d]:
                    part_in[d - 1, i] = jnp.zeros((rows, cols), part_in.dtype)
                else:
                    raw_a[d - 1, i] = jnp.zeros((rows, cols), raw_a.dtype)
                    raw_b[d - 1, i] = jnp.zeros((rows, cols), raw_b.dtype)

    @pl.when(col == 0)
    def _():
        first_load.start()

    @pl.when(col == 1)
    def _():
        first[...] = jnp.zeros(first.shape, first.dtype)

    @pl.when(jnp.logical_not(pair_due))
    def _():
        pair_in[...] = jnp.zeros(pair_in.shape, pair_in.dtype)

    k_pad[...] = jnp.zeros(k_pad.shape, k_pad.dtype)
    for f in range(v_pad.shape[0]):
        v_pad[f, :, :half] = jnp.zeros((v_pad.shape[1], half), v_pad.dtype)
        v_pad[f, :, half:] = jnp.ones((v_pad.shape[1], half), v_pad.dtype)

    def weight(target, k):
        table = mix_v[...]
        at = (lax.broadcasted_iota(jnp.int32, table.shape, 0) == k) & (
            lax.broadcasted_iota(jnp.int32, table.shape, 1) == target
        )
        return jnp.sum(jnp.where(at, table, 0.0), keepdims=True)

    def relay(some):
        for d in steps:

            @pl.when(onward(d))
            def _():
                own_weight = weight(section + 8 * d, 2 * d)
                partner_weight = weight(section + 8 * d, 2 * d - 1 + 2 * col)
                if 0 in some:
                    even_load(d).wait()
                for i in some:
                    if i in SUMMED[d]:
                        cross_copy(d, i).wait_recv()
                        value = own_weight * even[d - 1, :, chunk(ORDER[i])].astype(jnp.float32)
                        value = value + partner_weight * cross_in[d - 1, i].astype(jnp.float32)
                        part_out[d - 1, i] = value.astype(jnp.bfloat16)
                        part_copy(d, i).start()

    def relay_pair(some):
        if 0 in some:

            @pl.when(col == 0)
            def _():
                first_load.wait()

            for d in (1, 3):

                @pl.when(inward(d))
                def _():
                    raw_wait(d, 1).wait_recv()

        @pl.when(pair_sent)
        def _():
            weights = {d: weight(partner, 2 * d + 1 - 2 * col) for d in (1, 3)}
            first_weight = weight(partner, 1)
            for i in some:
                value = first_weight * first[:, chunk(ORDER[i])].astype(jnp.float32)
                for d in (1, 3):
                    if i not in SUMMED[d]:
                        value = value + weights[d] * raw_b[d - 1, i].astype(jnp.float32)
                pair_out[i] = value.astype(jnp.bfloat16)
                pair_copy(i).start()

    def gather_past(i):
        @pl.when(pair_due)
        def _():
            pair_copy(i).wait_recv()

        for d in steps:
            arriving = part_copy(d, i) if i in SUMMED[d] else raw_copy(d, 0, i)

            @pl.when(inward(d))
            def _():
                arriving.wait_recv()

        value = pair_in[i].astype(jnp.float32)
        for d in steps:
            if i in SUMMED[d]:
                value = value + part_in[d - 1, i].astype(jnp.float32)
            else:
                value = value + weight(section, 2 * d) * raw_a[d - 1, i].astype(jnp.float32)
        past[ORDER[i]] = value

    scale = 1.0 / math.sqrt(HEAD_DIM)

    def project(spans):
        def places():
            done = 0
            for block, first_row, size in spans:
                where = pl.ds(pl.multiple_of(block * rows + first_row, size), size)
                yield where, slice(done, done + size)
                done += size

        def tokens():
            taken = [rows_all[block, at : at + size, :] for block, at, size in spans]
            return taken[0] if len(taken) == 1 else jnp.concatenate(taken, axis=0)

        def q_tile(j, carry):
            acc = jnp.dot(tokens(), w_all[j], preferred_element_type=jnp.float32)
            acc = acc.astype(jnp.bfloat16) * jnp.bfloat16(scale)
            for where, got in places():
                q_all[2 * j, where, :] = acc[got, :half]
                q_all[2 * j + 1, where, :] = acc[got, half:]
            return carry

        lax.fori_loop(0, q_tiles, q_tile, 0)
        acc = jnp.dot(tokens(), w_all[q_tiles], preferred_element_type=jnp.float32)
        acc = acc.astype(jnp.bfloat16).astype(jnp.float32)
        for values, padded in ((acc[:, :half], k_pad), (acc[:, half:], v_pad)):
            lane = lax.broadcasted_iota(jnp.int32, values.shape, 1)
            turned = pltpu.roll(values, HEAD_DIM, 1)
            low = lane < HEAD_DIM
            zero = jnp.zeros_like(values)
            forms = (
                jnp.where(low, values, zero),
                jnp.where(low, zero, turned),
                jnp.where(low, turned, zero),
                jnp.where(low, zero, values),
            )
            for f, form in enumerate(forms):
                for where, got in places():
                    padded[f, where, pl.ds(0, half)] = form[got].astype(jnp.bfloat16)

    pairs = q_all.shape[0]
    pairs_per_kv = pairs // (half // HEAD_DIM)

    def attend(block, wanted, first_row, size):
        for b in range(4):
            keys = (b + 1) * rows
            at = b * rows + first_row

            @pl.when(wanted & (block == b))
            def _():
                with jax.named_scope(f"att{b}_{size}"):
                    shape = (pairs_per_kv, size, rows)
                    seen = (
                        lax.broadcasted_iota(jnp.int32, shape, 1) + first_row
                        >= lax.broadcasted_iota(jnp.int32, shape, 2)
                    ).reshape(pairs_per_kv * size, rows)
                    for kv in range(pairs // pairs_per_kv):
                        group = slice(kv * pairs_per_kv, (kv + 1) * pairs_per_kv)
                        query = q_all[group, at : at + size, :]
                        query = query.reshape(pairs_per_kv * size, half)
                        total = None
                        for which in range(2):
                            scores = lax.dot_general(
                                query,
                                k_pad[kv * 2 + which, :keys, :],
                                (((1,), (1,)), ((), ())),
                                preferred_element_type=jnp.float32,
                            )
                            last = jnp.where(seen, scores[:, b * rows :], -1e30)
                            if b:
                                scores = jnp.concatenate([scores[:, : b * rows], last], axis=1)
                            else:
                                scores = last
                            top = jnp.max(scores, axis=-1, keepdims=True)
                            weights = jnp.exp(scores - top).astype(jnp.bfloat16)
                            term = jnp.dot(
                                weights,
                                v_pad[kv * 2 + which, :keys, :],
                                preferred_element_type=jnp.float32,
                            )
                            term = term[:, :half] * (1.0 / term[:, half:])
                            total = term if total is None else total + term
                        total = total.astype(jnp.bfloat16)
                        for i in range(pairs_per_kv):
                            p = kv * pairs_per_kv + i
                            heads[b, first_row : first_row + size, p * half : (p + 1) * half] = (
                                total[i * size : (i + 1) * size]
                            )

    def part(block, c, first_row=0, size=rows):
        taken = heads[block, first_row : first_row + size, :]
        acc = jnp.dot(taken, w_out[c], preferred_element_type=jnp.float32)
        return acc.astype(jnp.bfloat16)

    short = rows // 2

    def far_copy(c, h, way):
        at = pl.ds(h * short, short)
        return pltpu.make_async_remote_copy(
            src_ref=far_send.at[c, at],
            dst_ref=relay_in.at[c, at],
            send_sem=far_s,
            recv_sem=far_r.at[c],
            device_id={"tensor": to[way]},
            device_id_type=MESH,
        )

    def near_copy(way, c):
        return pltpu.make_async_remote_copy(
            src_ref=near_send.at[way, c],
            dst_ref=final_in.at[way, c],
            send_sem=near_s,
            recv_sem=near_r.at[c],
            device_id={"tensor": to[way]},
            device_id_type=MESH,
        )

    def out_copy(c):
        return pltpu.make_async_remote_copy(
            src_ref=mixed.at[c],
            dst_ref=out_hbm.at[0, :, pl.ds(pl.multiple_of(c * cols, cols), cols)],
            send_sem=out_s,
            recv_sem=out_r,
            device_id={"section": nxt},
            device_id_type=MESH,
        )

    for copy in loads:
        copy.wait()
    project(((me, 0, rows),))

    def arrived(way, p):
        place = rows_all.at[source[way], pl.ds(p * piece, piece)]
        return pltpu.make_async_remote_copy(
            src_ref=place,
            dst_ref=place,
            send_sem=ag_s.at[way],
            recv_sem=ag_r.at[way, p],
            device_id={"tensor": to[way]},
            device_id_type=MESH,
        )

    for p in range(PIECES):
        for way in range(2):
            arrived(way, p).wait_recv()
            pass_copy(way, p).start()
        if p == 1:
            load_mix.wait()
            with jax.named_scope("relay0"):
                relay((0,))
    with jax.named_scope("relay1"):
        relay((1,))
    for copy in out_loads:
        copy.wait()
    with jax.named_scope("f_proj_near"):
        project(((left, 0, rows), (right, 0, rows)))
    attend(me, far > me, 0, rows)

    for h in range(2):
        settle(rows_all.at[far, pl.ds(h * short, short)], fw_s.at[0], fw_r.at[h]).wait_recv()
        with jax.named_scope(f"i_proj_far{h}"):
            project(((far, h * short, short),))
        with jax.named_scope(f"j_att_far{h}"):
            attend(far, True, h * short, short)

        def far_step(i, carry):
            at = pl.ds(h * short, short)
            far_send[i, at] = part(far, i, h * short, short)
            far_copy(i, h, 1).start()
            far_send[side + i, at] = part(far, side + i, h * short, short)
            far_copy(side + i, h, 0).start()
            return carry

        with jax.named_scope(f"k_far_step{h}"):
            lax.fori_loop(0, side, far_step, 0)
        if h == 0:
            with jax.named_scope("relay2"):
                relay((2, 3, 4))
            with jax.named_scope("relay_pair"):
                relay_pair((0, 1, 2, 3))

    attend(right, True, 0, rows)
    attend(left, True, 0, rows)
    with jax.named_scope("relay3"):
        relay((5, 6, 7))
        relay_pair((4, 5, 6, 7))

    def near_step(i, carry):
        def relayed(way):
            c = side + i if way == 0 else i
            value = part(to[way], c)
            settle(relay_in.at[c], far_s, far_r.at[c]).wait_recv()
            total = value.astype(jnp.float32) + relay_in[c].astype(jnp.float32)
            near_send[way, c] = total.astype(jnp.bfloat16)
            near_copy(way, c).start()

        def direct(way):
            c = i if way == 0 else side + i
            near_send[way, c] = part(to[way], c)
            near_copy(way, c).start()

        relayed(0)
        direct(1)
        relayed(1)
        direct(0)
        return carry

    lax.fori_loop(0, side, near_step, 0)
    attend(me, far < me, 0, rows)

    def own_step(c, carry):
        own_part[c] = part(me, c)
        return carry

    lax.fori_loop(0, col_chunks, own_step, 0)

    own_weight = weight(section, 0)

    for i in range(col_chunks):
        c = ORDER[i]
        with jax.named_scope(f"past{i}"):
            gather_past(i)
        with jax.named_scope(f"final{i}"):
            total = own_part[c].astype(jnp.float32)
            settle(final_in.at[:, c], near_s, near_r.at[c]).wait_recv()
            for way in range(2):
                total = total + final_in[way, c].astype(jnp.float32)
            block = (x_own[:, chunk(c)].astype(jnp.float32) + total).astype(jnp.bfloat16)
            mixed[c] = (own_weight * block.astype(jnp.float32) + past[c]).astype(jnp.bfloat16)
            out_copy(c).start()
    for way in range(2):
        settle(rows_all.at[me], ag_s.at[way], ag_r.at[way, 0]).wait_send()
        half_block = rows_all.at[me, :, pl.ds(0, width // 2)]
        settle(half_block, fw_s.at[way], fw_r.at[0]).wait_send()

    for d in steps:

        @pl.when(onward(d))
        def _():
            sent = pl.ds(SUMMED[d].start, len(SUMMED[d]))
            settle(cross_in.at[d - 1, sent], cross_s.at[d - 1], cross_r.at[0, 0]).wait_send()
            settle(part_out.at[d - 1, sent], part_s.at[d - 1], part_r.at[0, 0]).wait_send()
            if d in PLAIN:
                raw_wait(d, 0).wait_send()
                raw_wait(d, 1).wait_send()

    @pl.when(pair_sent)
    def _():
        settle(pair_out, pair_s, pair_r.at[0]).wait_send()

    settle(far_send, far_s, far_r.at[0]).wait_send()
    settle(near_send, near_s, near_r.at[0]).wait_send()
    with jax.named_scope("s_drain"):
        settle(mixed, out_s, out_r).wait_send()
        settle(out_hbm.at[0], out_s, out_r).wait_recv()


def solution(mesh):
    sections, tensor = mesh.shape["section"], mesh.shape["tensor"]
    assert tensor == 4 and sections == 32
    col_chunks = 8

    def on_device(x, history, wq, wk, wv, wo, mix_weights):
        rows, width = x.shape[1:]
        q_width, kv_width = wq.shape[2], wk.shape[2]
        seq = rows * tensor
        tile = 2 * kv_width
        q_tiles = q_width // tile
        cols = width // col_chunks
        bf16 = jnp.bfloat16
        dma = pltpu.SemaphoreType.DMA
        hbm = pl.BlockSpec(memory_space=pl.ANY)
        return pl.pallas_call(
            functools.partial(tick_kernel, sections),
            out_shape=pltpu.VMEM(x.shape, bf16),
            in_specs=[hbm] * 7,
            out_specs=hbm,
            scratch_shapes=[
                pltpu.VMEM((rows, width), bf16),
                pltpu.VMEM((tensor, rows, width), bf16),
                pltpu.VMEM((q_tiles + 1, width, tile), bf16),
                pltpu.VMEM((col_chunks, q_width, cols), bf16),
                pltpu.VMEM((2 * q_tiles, seq, kv_width), bf16),
                pltpu.VMEM((4, seq, kv_width), bf16),
                pltpu.VMEM((4, seq, 2 * kv_width), bf16),
                pltpu.VMEM((tensor, rows, q_width), bf16),
                pltpu.VMEM((col_chunks, rows, cols), bf16),
                pltpu.VMEM((col_chunks, rows, cols), bf16),
                pltpu.VMEM((2, col_chunks, rows, cols), bf16),
                pltpu.VMEM((2, col_chunks, rows, cols), bf16),
                pltpu.VMEM((col_chunks, rows, cols), bf16),
                pltpu.VMEM((col_chunks, rows, cols), bf16),
                pltpu.VMEM((3, rows, width), bf16),
                pltpu.VMEM((3, col_chunks, rows, cols), bf16),
                pltpu.VMEM((3, col_chunks, rows, cols), bf16),
                pltpu.VMEM((3, col_chunks, rows, cols), bf16),
                pltpu.VMEM((3, col_chunks, rows, cols), bf16),
                pltpu.VMEM((3, col_chunks, rows, cols), bf16),
                pltpu.VMEM((rows, width), bf16),
                pltpu.VMEM((col_chunks, rows, cols), bf16),
                pltpu.VMEM((col_chunks, rows, cols), bf16),
                pltpu.VMEM((col_chunks, rows, cols), jnp.float32),
                pltpu.VMEM(mix_weights.shape[::-1], mix_weights.dtype),
                dma((q_tiles + 2,)),
                dma((col_chunks,)),
                dma((PIECES,)),
                dma,
                dma((3,)),
                dma,
                dma((3,)),
                dma((3, col_chunks)),
                dma((3,)),
                dma((3, col_chunks)),
                dma((2, 3)),
                dma((3, col_chunks + 1)),
                dma,
                dma((col_chunks,)),
                dma((2,)),
                dma((2, PIECES)),
                dma((2,)),
                dma((2,)),
                dma,
                dma((col_chunks,)),
                dma,
                dma((col_chunks,)),
                dma,
                dma,
            ],
            compiler_params=pltpu.CompilerParams(
                collective_id=0, has_side_effects=True, vmem_limit_bytes=60 * 1024 * 1024
            ),
        )(x, history, wq, wk, wv, wo, mix_weights.T)

    placed = (
        P("section", "tensor", None),
        P("section", None, "tensor", None),
        P("section", None, "tensor"),
        P("section", None, "tensor"),
        P("section", None, "tensor"),
        P("section", "tensor", None),
        P(),
    )
    return jax.shard_map(
        on_device,
        mesh=mesh,
        in_specs=placed,
        out_specs=P("section", "tensor", None),
        check_vma=False,
    )
```

```python
import functools
import math

import jax
import jax.numpy as jnp
from jax import lax
from jax.experimental import pallas as pl
from jax.experimental.pallas import tpu as pltpu
from jax.sharding import PartitionSpec as P

HEAD_DIM = 64
ORDER = (4, 0, 5, 1, 6, 2, 7, 3)
SUMMED = {1: range(0, 3), 2: range(0, 8), 3: range(6, 8)}
PLAIN = {1: range(3, 8), 3: range(0, 6)}
SUMMED_AT = {1: 0, 2: 3, 3: 5}
PLAIN_AT = {1: -3, 3: 5}
MESH = pl.DeviceIdType.MESH
PIECES = 4


def start(copy):
    copy.start()
    return copy


def tick_kernel(
    sections,
    x_hbm,
    hist_hbm,
    wq_hbm,
    wk_hbm,
    wv_hbm,
    wo_hbm,
    mix_hbm,
    out_hbm,
    x_own,
    rows_all,
    w_all,
    w_out,
    q_all,
    k_pad,
    v_pad,
    heads,
    far_send,
    relay_in,
    near_send,
    final_in,
    own_part,
    mixed,
    even,
    cross_in,
    part_out,
    part_in,
    raw_a,
    raw_b,
    first,
    pair_out,
    pair_in,
    past,
    mix_v,
    w_sem,
    wo_sem,
    x_sem,
    mix_sem,
    even_sem,
    first_sem,
    cross_s,
    cross_r,
    part_s,
    part_r,
    raw_s,
    raw_r,
    pair_s,
    pair_r,
    ag_s,
    ag_r,
    fw_s,
    fw_r,
    far_s,
    far_r,
    near_s,
    near_r,
    out_s,
    out_r,
):
    section = lax.axis_index("section")
    me = lax.axis_index("tensor")
    right, left, far = lax.rem(me + 1, 4), lax.rem(me + 3, 4), lax.rem(me + 2, 4)
    to = (right, left)
    source = (left, right)
    rows, width = x_own.shape
    piece = rows // PIECES
    q_tiles = w_all.shape[0] - 1
    tile = w_all.shape[2]
    half = tile // 2
    col_chunks, _, cols = w_out.shape
    side = col_chunks // 2
    nxt = lax.rem(section + 1, sections)
    prv = lax.rem(section + sections - 1, sections)

    def load_x(p):
        at = pl.ds(p * piece, piece)
        return pltpu.make_async_copy(x_hbm.at[0, at], x_own.at[at], x_sem.at[p])

    for p in range(PIECES):
        load_x(p).start()
    barrier = pltpu.get_barrier_semaphore()
    for other in to:
        pl.semaphore_signal(barrier, inc=1, device_id={"tensor": other}, device_id_type=MESH)
    row, col = section // 8, lax.rem(section // 4, 2)
    partner = section + 4 - 8 * col
    others = [lax.rem(section + 8 * d, sections) for d in (1, 2, 3)]
    for other in (nxt, prv, partner, *others):
        pl.semaphore_signal(barrier, inc=1, device_id={"section": other}, device_id_type=MESH)

    loads = []
    for j in range(q_tiles):
        loads.append(
            pltpu.make_async_copy(
                wq_hbm.at[0, :, pl.ds(j * tile, tile)], w_all.at[j], w_sem.at[j]
            )
        )
    loads.append(
        pltpu.make_async_copy(
            wk_hbm.at[0], w_all.at[q_tiles, :, pl.ds(0, half)], w_sem.at[q_tiles]
        )
    )
    loads.append(
        pltpu.make_async_copy(
            wv_hbm.at[0], w_all.at[q_tiles, :, pl.ds(half, half)], w_sem.at[q_tiles + 1]
        )
    )
    load_x(0).wait()
    for copy in loads:
        copy.start()
    load_mix = start(pltpu.make_async_copy(mix_hbm, mix_v, mix_sem))

    def own_copy(way, p):
        place = rows_all.at[me, pl.ds(p * piece, piece)]
        return pltpu.make_async_remote_copy(
            src_ref=place,
            dst_ref=place,
            send_sem=ag_s.at[way],
            recv_sem=ag_r.at[way, p],
            device_id={"tensor": to[way]},
            device_id_type=MESH,
        )

    def settle(ref, send, recv):
        return pltpu.make_async_remote_copy(
            src_ref=ref,
            dst_ref=ref,
            send_sem=send,
            recv_sem=recv,
            device_id={"tensor": right},
            device_id_type=MESH,
        )

    def passed(way, p, block):
        place = rows_all.at[
            block, pl.ds(p * piece, piece), pl.ds(way * (width // 2), width // 2)
        ]
        return pltpu.make_async_remote_copy(
            src_ref=place,
            dst_ref=place,
            send_sem=fw_s.at[way],
            recv_sem=fw_r.at[p // 2],
            device_id={"tensor": to[way]},
            device_id_type=MESH,
        )

    def pass_copy(way, p):
        return passed(way, p, source[way])

    def norm_piece(p):
        def norm_rows(i, carry):
            at = pl.ds(pl.multiple_of(p * piece + i * 16, 16), 16)
            values = x_own[at, :].astype(jnp.float32)
            inv = lax.rsqrt(jnp.mean(values * values, axis=-1, keepdims=True) + 1e-05)
            rows_all[me, at, :] = (values * inv).astype(jnp.bfloat16)
            return carry

        lax.fori_loop(0, piece // 16, norm_rows, 0)

    norm_piece(0)
    pl.semaphore_wait(barrier, 8)
    own_copy(0, 0).start()
    own_copy(1, 0).start()

    steps = range(1, 4)

    def chunk(c):
        return pl.ds(c * cols, cols)

    def onward(d):
        return row + d < 4

    def inward(d):
        return row >= d

    def section_copy(src, dst, send, recv, target):
        return pltpu.make_async_remote_copy(
            src_ref=src,
            dst_ref=dst,
            send_sem=send,
            recv_sem=recv,
            device_id={"section": target},
            device_id_type=MESH,
        )

    def cross_copy(d, i):
        return section_copy(
            hist_hbm.at[0, jnp.maximum(2 * d - 2 * col, 0), :, chunk(ORDER[i])],
            cross_in.at[d - 1, i],
            cross_s.at[d - 1],
            cross_r.at[SUMMED_AT[d] + i],
            partner,
        )

    def part_copy(d, i):
        return section_copy(
            part_out.at[d - 1, i],
            part_in.at[d - 1, i],
            part_s.at[d - 1],
            part_r.at[SUMMED_AT[d] + i],
            others[d - 1],
        )

    def raw_copy(d, which, i):
        slot = 2 * d - 1 if which == 0 else 2 * d - 2 * col
        return section_copy(
            hist_hbm.at[0, slot, :, chunk(ORDER[i])],
            (raw_a, raw_b)[which].at[d - 1, i],
            raw_s.at[which, d - 1],
            raw_r.at[PLAIN_AT[d] + i if which == 0 else 11 + d // 2],
            others[d - 1],
        )

    def plain(d):
        return pl.ds(PLAIN[d].start, len(PLAIN[d]))

    def raw_wait(d, which):
        raw = (raw_a, raw_b)[which].at[d - 1, plain(d)]
        return settle(raw, raw_s.at[which, d - 1], raw_r.at[11 + d // 2])

    def pair_copy(i):
        return section_copy(pair_out.at[i], pair_in.at[i], pair_s, pair_r.at[i], partner)

    pair_sent = (row >= 1) | (col == 0)
    pair_due = (row >= 1) | (col == 1)

    def even_load(d):
        return pltpu.make_async_copy(
            hist_hbm.at[0, 2 * d - 1], even.at[d - 1], even_sem.at[d - 1]
        )

    first_load = pltpu.make_async_copy(hist_hbm.at[0, 0], first, first_sem)

    for i in range(col_chunks):
        for d in steps:
            if i in SUMMED[d]:

                @pl.when(onward(d))
                def _():
                    cross_copy(d, i).start()

    for which in (1, 0):
        for d in (1, 3):

            @pl.when(onward(d))
            def _():
                for i in PLAIN[d]:
                    raw_copy(d, which, i).start()

    for p in range(1, PIECES):
        load_x(p).wait()
        norm_piece(p)
        own_copy(0, p).start()
        own_copy(1, p).start()

    out_loads = []
    for c in range(col_chunks):
        out_loads.append(
            start(
                pltpu.make_async_copy(
                    wo_hbm.at[0, :, pl.ds(c * cols, cols)], w_out.at[c], wo_sem.at[c]
                )
            )
        )

    for d in steps:

        @pl.when(onward(d))
        def _():
            even_load(d).start()

        @pl.when(row < d)
        def _():
            for i in range(col_chunks):
                if i in SUMMED[d]:
                    part_in[d - 1, i] = jnp.zeros((rows, cols), part_in.dtype)
                else:
                    raw_a[d - 1, i] = jnp.zeros((rows, cols), raw_a.dtype)
                    raw_b[d - 1, i] = jnp.zeros((rows, cols), raw_b.dtype)

    @pl.when(col == 0)
    def _():
        first_load.start()

    @pl.when(col == 1)
    def _():
        first[...] = jnp.zeros(first.shape, first.dtype)

    @pl.when(jnp.logical_not(pair_due))
    def _():
        pair_in[...] = jnp.zeros(pair_in.shape, pair_in.dtype)

    k_pad[...] = jnp.zeros(k_pad.shape, k_pad.dtype)
    for f in range(v_pad.shape[0]):
        v_pad[f, :, :half] = jnp.zeros((v_pad.shape[1], half), v_pad.dtype)
        v_pad[f, :, half:] = jnp.ones((v_pad.shape[1], half), v_pad.dtype)

    def weight(target, k):
        table = mix_v[...]
        at = (lax.broadcasted_iota(jnp.int32, table.shape, 0) == k) & (
            lax.broadcasted_iota(jnp.int32, table.shape, 1) == target
        )
        return jnp.sum(jnp.where(at, table, 0.0), keepdims=True)

    def relay(some):
        for d in steps:

            @pl.when(onward(d))
            def _():
                own_weight = weight(section + 8 * d, 2 * d)
                partner_weight = weight(section + 8 * d, 2 * d - 1 + 2 * col)
                if 0 in some:
                    even_load(d).wait()
                for i in some:
                    if i in SUMMED[d]:
                        cross_copy(d, i).wait_recv()
                        value = own_weight * even[d - 1, :, chunk(ORDER[i])].astype(jnp.float32)
                        value = value + partner_weight * cross_in[d - 1, i].astype(jnp.float32)
                        part_out[d - 1, i] = value.astype(jnp.bfloat16)
                        part_copy(d, i).start()

    def relay_pair(some):
        if 0 in some:

            @pl.when(col == 0)
            def _():
                first_load.wait()

            for d in (1, 3):

                @pl.when(inward(d))
                def _():
                    raw_wait(d, 1).wait_recv()

        @pl.when(pair_sent)
        def _():
            weights = {d: weight(partner, 2 * d + 1 - 2 * col) for d in (1, 3)}
            first_weight = weight(partner, 1)
            for i in some:
                value = first_weight * first[:, chunk(ORDER[i])].astype(jnp.float32)
                for d in (1, 3):
                    if i not in SUMMED[d]:
                        value = value + weights[d] * raw_b[d - 1, i].astype(jnp.float32)
                pair_out[i] = value.astype(jnp.bfloat16)
                pair_copy(i).start()

    def gather_past(i):
        @pl.when(pair_due)
        def _():
            pair_copy(i).wait_recv()

        for d in steps:
            arriving = part_copy(d, i) if i in SUMMED[d] else raw_copy(d, 0, i)

            @pl.when(inward(d))
            def _():
                arriving.wait_recv()

        value = pair_in[i].astype(jnp.float32)
        for d in steps:
            if i in SUMMED[d]:
                value = value + part_in[d - 1, i].astype(jnp.float32)
            else:
                value = value + weight(section, 2 * d) * raw_a[d - 1, i].astype(jnp.float32)
        past[ORDER[i]] = value

    scale = 1.0 / math.sqrt(HEAD_DIM)

    def project(spans):
        def places():
            done = 0
            for block, first_row, size in spans:
                where = pl.ds(pl.multiple_of(block * rows + first_row, size), size)
                yield where, slice(done, done + size)
                done += size

        def tokens():
            taken = [rows_all[block, at : at + size, :] for block, at, size in spans]
            return taken[0] if len(taken) == 1 else jnp.concatenate(taken, axis=0)

        def q_tile(j, carry):
            acc = jnp.dot(tokens(), w_all[j], preferred_element_type=jnp.float32)
            acc = acc.astype(jnp.bfloat16) * jnp.bfloat16(scale)
            for where, got in places():
                q_all[2 * j, where, :] = acc[got, :half]
                q_all[2 * j + 1, where, :] = acc[got, half:]
            return carry

        lax.fori_loop(0, q_tiles, q_tile, 0)
        acc = jnp.dot(tokens(), w_all[q_tiles], preferred_element_type=jnp.float32)
        acc = acc.astype(jnp.bfloat16).astype(jnp.float32)
        for values, padded in ((acc[:, :half], k_pad), (acc[:, half:], v_pad)):
            lane = lax.broadcasted_iota(jnp.int32, values.shape, 1)
            turned = pltpu.roll(values, HEAD_DIM, 1)
            low = lane < HEAD_DIM
            zero = jnp.zeros_like(values)
            forms = (
                jnp.where(low, values, zero),
                jnp.where(low, zero, turned),
                jnp.where(low, turned, zero),
                jnp.where(low, zero, values),
            )
            for f, form in enumerate(forms):
                for where, got in places():
                    padded[f, where, pl.ds(0, half)] = form[got].astype(jnp.bfloat16)

    pairs = q_all.shape[0]
    pairs_per_kv = pairs // (half // HEAD_DIM)

    def attend(block, wanted, first_row, size):
        for b in range(4):
            keys = (b + 1) * rows
            at = b * rows + first_row

            @pl.when(wanted & (block == b))
            def _():
                with jax.named_scope(f"att{b}_{size}"):
                    shape = (pairs_per_kv, size, rows)
                    seen = (
                        lax.broadcasted_iota(jnp.int32, shape, 1) + first_row
                        >= lax.broadcasted_iota(jnp.int32, shape, 2)
                    ).reshape(pairs_per_kv * size, rows)
                    for kv in range(pairs // pairs_per_kv):
                        group = slice(kv * pairs_per_kv, (kv + 1) * pairs_per_kv)
                        query = q_all[group, at : at + size, :]
                        query = query.reshape(pairs_per_kv * size, half)
                        total = None
                        for which in range(2):
                            scores = lax.dot_general(
                                query,
                                k_pad[kv * 2 + which, :keys, :],
                                (((1,), (1,)), ((), ())),
                                preferred_element_type=jnp.float32,
                            )
                            last = jnp.where(seen, scores[:, b * rows :], -1e30)
                            if b:
                                scores = jnp.concatenate([scores[:, : b * rows], last], axis=1)
                            else:
                                scores = last
                            top = jnp.max(scores, axis=-1, keepdims=True)
                            weights = jnp.exp(scores - top).astype(jnp.bfloat16)
                            term = jnp.dot(
                                weights,
                                v_pad[kv * 2 + which, :keys, :],
                                preferred_element_type=jnp.float32,
                            )
                            term = term[:, :half] * (1.0 / term[:, half:])
                            total = term if total is None else total + term
                        total = total.astype(jnp.bfloat16)
                        for i in range(pairs_per_kv):
                            p = kv * pairs_per_kv + i
                            heads[b, first_row : first_row + size, p * half : (p + 1) * half] = (
                                total[i * size : (i + 1) * size]
                            )

    def part(block, c, first_row=0, size=rows):
        taken = heads[block, first_row : first_row + size, :]
        acc = jnp.dot(taken, w_out[c], preferred_element_type=jnp.float32)
        return acc.astype(jnp.bfloat16)

    short = rows // 2

    def far_copy(c, h, way):
        at = pl.ds(h * short, short)
        return pltpu.make_async_remote_copy(
            src_ref=far_send.at[c, at],
            dst_ref=relay_in.at[c, at],
            send_sem=far_s,
            recv_sem=far_r.at[c],
            device_id={"tensor": to[way]},
            device_id_type=MESH,
        )

    def near_copy(way, c):
        return pltpu.make_async_remote_copy(
            src_ref=near_send.at[way, c],
            dst_ref=final_in.at[way, c],
            send_sem=near_s,
            recv_sem=near_r.at[c],
            device_id={"tensor": to[way]},
            device_id_type=MESH,
        )

    def out_copy(c):
        return pltpu.make_async_remote_copy(
            src_ref=mixed.at[c],
            dst_ref=out_hbm.at[0, :, pl.ds(pl.multiple_of(c * cols, cols), cols)],
            send_sem=out_s,
            recv_sem=out_r,
            device_id={"section": nxt},
            device_id_type=MESH,
        )

    for copy in loads:
        copy.wait()
    project(((me, 0, rows),))

    def arrived(way, p):
        place = rows_all.at[source[way], pl.ds(p * piece, piece)]
        return pltpu.make_async_remote_copy(
            src_ref=place,
            dst_ref=place,
            send_sem=ag_s.at[way],
            recv_sem=ag_r.at[way, p],
            device_id={"tensor": to[way]},
            device_id_type=MESH,
        )

    for p in range(PIECES):
        for way in range(2):
            arrived(way, p).wait_recv()
            pass_copy(way, p).start()
        if p == 1:
            load_mix.wait()
            with jax.named_scope("relay0"):
                relay((0,))
    with jax.named_scope("relay1"):
        relay((1,))
    for copy in out_loads:
        copy.wait()
    with jax.named_scope("f_proj_near"):
        project(((left, 0, rows), (right, 0, rows)))
    attend(me, far > me, 0, rows)

    for h in range(2):
        settle(rows_all.at[far, pl.ds(h * short, short)], fw_s.at[0], fw_r.at[h]).wait_recv()
        with jax.named_scope(f"i_proj_far{h}"):
            project(((far, h * short, short),))
        with jax.named_scope(f"j_att_far{h}"):
            attend(far, True, h * short, short)

        def far_step(i, carry):
            at = pl.ds(h * short, short)
            far_send[i, at] = part(far, i, h * short, short)
            far_copy(i, h, 1).start()
            far_send[side + i, at] = part(far, side + i, h * short, short)
            far_copy(side + i, h, 0).start()
            return carry

        with jax.named_scope(f"k_far_step{h}"):
            lax.fori_loop(0, side, far_step, 0)
        if h == 0:
            with jax.named_scope("relay2"):
                relay((2, 3, 4))
            with jax.named_scope("relay_pair"):
                relay_pair((0, 1, 2, 3))

    attend(right, True, 0, rows)
    attend(left, True, 0, rows)
    with jax.named_scope("relay3"):
        relay((5, 6, 7))
        relay_pair((4, 5, 6, 7))

    def near_step(i, carry):
        def relayed(way):
            c = side + i if way == 0 else i
            value = part(to[way], c)
            settle(relay_in.at[c], far_s, far_r.at[c]).wait_recv()
            total = value.astype(jnp.float32) + relay_in[c].astype(jnp.float32)
            near_send[way, c] = total.astype(jnp.bfloat16)
            near_copy(way, c).start()

        def direct(way):
            c = i if way == 0 else side + i
            near_send[way, c] = part(to[way], c)
            near_copy(way, c).start()

        relayed(0)
        direct(1)
        relayed(1)
        direct(0)
        return carry

    lax.fori_loop(0, side, near_step, 0)
    attend(me, far < me, 0, rows)

    def own_step(c, carry):
        own_part[c] = part(me, c)
        return carry

    lax.fori_loop(0, col_chunks, own_step, 0)

    own_weight = weight(section, 0)

    for i in range(col_chunks):
        c = ORDER[i]
        with jax.named_scope(f"past{i}"):
            gather_past(i)
        with jax.named_scope(f"final{i}"):
            total = own_part[c].astype(jnp.float32)
            settle(final_in.at[:, c], near_s, near_r.at[c]).wait_recv()
            for way in range(2):
                total = total + final_in[way, c].astype(jnp.float32)
            block = (x_own[:, chunk(c)].astype(jnp.float32) + total).astype(jnp.bfloat16)
            mixed[c] = (own_weight * block.astype(jnp.float32) + past[c]).astype(jnp.bfloat16)
            out_copy(c).start()
    for way in range(2):
        settle(rows_all.at[me], ag_s.at[way], ag_r.at[way, 0]).wait_send()
        half_block = rows_all.at[me, :, pl.ds(0, width // 2)]
        settle(half_block, fw_s.at[way], fw_r.at[0]).wait_send()

    for d in steps:

        @pl.when(onward(d))
        def _():
            sent = pl.ds(SUMMED[d].start, len(SUMMED[d]))
            settle(cross_in.at[d - 1, sent], cross_s.at[d - 1], cross_r.at[0]).wait_send()
            settle(part_out.at[d - 1, sent], part_s.at[d - 1], part_r.at[0]).wait_send()
            if d in PLAIN:
                raw_wait(d, 0).wait_send()
                raw_wait(d, 1).wait_send()

    @pl.when(pair_sent)
    def _():
        settle(pair_out, pair_s, pair_r.at[0]).wait_send()

    settle(far_send, far_s, far_r.at[0]).wait_send()
    settle(near_send, near_s, near_r.at[0]).wait_send()
    with jax.named_scope("s_drain"):
        settle(mixed, out_s, out_r).wait_send()
        settle(out_hbm.at[0], out_s, out_r).wait_recv()


def solution(mesh):
    sections, tensor = mesh.shape["section"], mesh.shape["tensor"]
    assert tensor == 4 and sections == 32
    col_chunks = 8

    def on_device(x, history, wq, wk, wv, wo, mix_weights):
        rows, width = x.shape[1:]
        q_width, kv_width = wq.shape[2], wk.shape[2]
        seq = rows * tensor
        tile = 2 * kv_width
        q_tiles = q_width // tile
        cols = width // col_chunks
        bf16 = jnp.bfloat16
        dma = pltpu.SemaphoreType.DMA
        hbm = pl.BlockSpec(memory_space=pl.ANY)
        return pl.pallas_call(
            functools.partial(tick_kernel, sections),
            out_shape=pltpu.VMEM(x.shape, bf16),
            in_specs=[hbm] * 7,
            out_specs=hbm,
            scratch_shapes=[
                pltpu.VMEM((rows, width), bf16),
                pltpu.VMEM((tensor, rows, width), bf16),
                pltpu.VMEM((q_tiles + 1, width, tile), bf16),
                pltpu.VMEM((col_chunks, q_width, cols), bf16),
                pltpu.VMEM((2 * q_tiles, seq, kv_width), bf16),
                pltpu.VMEM((4, seq, kv_width), bf16),
                pltpu.VMEM((4, seq, 2 * kv_width), bf16),
                pltpu.VMEM((tensor, rows, q_width), bf16),
                pltpu.VMEM((col_chunks, rows, cols), bf16),
                pltpu.VMEM((col_chunks, rows, cols), bf16),
                pltpu.VMEM((2, col_chunks, rows, cols), bf16),
                pltpu.VMEM((2, col_chunks, rows, cols), bf16),
                pltpu.VMEM((col_chunks, rows, cols), bf16),
                pltpu.VMEM((col_chunks, rows, cols), bf16),
                pltpu.VMEM((3, rows, width), bf16),
                pltpu.VMEM((3, col_chunks, rows, cols), bf16),
                pltpu.VMEM((3, col_chunks, rows, cols), bf16),
                pltpu.VMEM((3, col_chunks, rows, cols), bf16),
                pltpu.VMEM((3, col_chunks, rows, cols), bf16),
                pltpu.VMEM((3, col_chunks, rows, cols), bf16),
                pltpu.VMEM((rows, width), bf16),
                pltpu.VMEM((col_chunks, rows, cols), bf16),
                pltpu.VMEM((col_chunks, rows, cols), bf16),
                pltpu.VMEM((col_chunks, rows, cols), jnp.float32),
                pltpu.VMEM(mix_weights.shape[::-1], mix_weights.dtype),
                dma((q_tiles + 2,)),
                dma((col_chunks,)),
                dma((PIECES,)),
                dma,
                dma((3,)),
                dma,
                dma((3,)),
                dma((13,)),
                dma((3,)),
                dma((13,)),
                dma((2, 3)),
                dma((13,)),
                dma,
                dma((col_chunks,)),
                dma((2,)),
                dma((2, PIECES)),
                dma((2,)),
                dma((2,)),
                dma,
                dma((col_chunks,)),
                dma,
                dma((col_chunks,)),
                dma,
                dma,
            ],
            compiler_params=pltpu.CompilerParams(
                collective_id=0, has_side_effects=True, vmem_limit_bytes=60 * 1024 * 1024
            ),
        )(x, history, wq, wk, wv, wo, mix_weights.T)

    placed = (
        P("section", "tensor", None),
        P("section", None, "tensor", None),
        P("section", None, "tensor"),
        P("section", None, "tensor"),
        P("section", None, "tensor"),
        P("section", "tensor", None),
        P(),
    )
    return jax.shard_map(
        on_device,
        mesh=mesh,
        in_specs=placed,
        out_specs=P("section", "tensor", None),
        check_vma=False,
    )
```
